768 devices in a mesh: dp: 32 (over z_hi, y, core), tensor: 24 (over z_lo, x).
Axes of the slice: x: 4, y: 8, z: 12 (z_hi: 2, z_lo: 6; z = z_hi * 6 + z_lo), core: 2. Of those that a mesh axis runs over, the one named last changes fastest.
Arguments:
- tokens: bfloat16 [1024, 6144], P('dp', 'tensor'), may hold values from -6 to 6
- router_weight: bfloat16 [6144, 8], P('tensor'), may hold values from -0.078125 to 0.078125
- expert_ids: int32 [1024, 2], P('dp'), may hold values from 0 to 7, all different within a row; in each aligned block of 32 rows (0 to 31, 32 to 63, ...) at most 12 rows name the same one
- w_gate: bfloat16 [32, 6144, 3072], P('dp', None, 'tensor'), may hold values from -0.078125 to 0.078125
- w_up: bfloat16 [32, 6144, 3072], P('dp', None, 'tensor'), may hold values from -0.078125 to 0.078125
- w_down: bfloat16 [32, 3072, 6144], P('dp', 'tensor'), may hold values from -0.0546875 to 0.0546875
Outputs:
- moe_out: bfloat16 [1024, 6144], P('dp', 'tensor')
The draws below stay inside these ranges and needn't reach their ends.
Inputs may be any that keep to these rules, and one draw needn't show every extreme that they name: `expert_ids`: the two experts of a token differ. In each aligned block of 32 rows (the rows of one index of dp) no expert is named by more than 12 rows, a bound that some blocks reach.
All inputs are finite; a program needn't handle non-finite values.
Results may differ from the reference program's by a relative error of at most 0.022.
Values may be sent and summed in bfloat16 or wider, within the bound.
No kernel may reach another device: no remote copies, remote signals or barrier semaphores. Data moves between devices by JAX's collectives and lax.ppermute only.
A program may use at most 32 MiB of HBM per device.

```python
import math
import jax
import jax.numpy as jnp
import numpy as np
from jax import lax

D = 6144
FF = 12288
EXPERTS = 8
TOK_DP = 32
CAP = 12
TOKENS = 1024
N_DP = 32
N_TENSOR = 24


def block_scale(stream_key, dims, cuts, low, high):
    level, own = 1.0, jax.random.fold_in(stream_key, 6)
    for dim, blocks in cuts:
        draws = jnp.exp(jax.random.uniform(jax.random.fold_in(own, dim), (blocks,), jnp.float32, low / len(cuts), high / len(cuts)))
        level = level * jnp.repeat(draws, dims[dim] // blocks).reshape([-1 if axis == dim else 1 for axis in range(len(dims))])
    return level


def assign_block(rng, own, number, rows, amount, top, bound, slope):
    ranking = jax.random.permutation(rng, amount)
    packed, ordinary = portions_of(amount, rows * top, bound, slope, True), portions_of(amount, rows * top, bound, slope, False)
    places = jnp.arange(amount)

    def named(lengths, offset_by):
        used = int((lengths > 0).sum())
        fixed = max(1, used // 4)
        moved = fixed + (places - fixed + offset_by * (used - fixed)) % max(1, amount - fixed)
        return jnp.zeros((amount,), jnp.int32).at[ranking[jnp.where(places < fixed, places, moved)]].set(jnp.asarray(lengths, jnp.int32))

    lengths = jnp.where(number % 4 == 0, named(packed, number // 4), named(ordinary, number - number // 4 - 1))
    mixed = jax.random.permutation(jax.random.fold_in(own, 3), amount)
    donor, taker = mixed[0:amount // 2 * 2:2], mixed[1:amount // 2 * 2:2]
    slack = jnp.minimum(lengths[donor] - 1, bound - lengths[taker]) // 2
    slack = jnp.where((donor == ranking[0]) | (taker == ranking[0]) | (lengths[taker] == 0), 0, jnp.maximum(slack, 0))
    moved = jax.random.randint(jax.random.fold_in(own, 4), (amount // 2,), 0, 1 << 20) % (slack + 1)
    lengths = lengths.at[donor].add(-moved).at[taker].add(moved)
    labels = jnp.searchsorted(jnp.cumsum(lengths), jnp.arange(rows * top), side="right").astype(jnp.int32)
    grid = labels.reshape(top, rows).T
    grid = grid[jax.random.permutation(jax.random.fold_in(own, 1), rows)]
    offset_by = jax.random.randint(jax.random.fold_in(own, 2), (rows, 1), 0, top)
    return jnp.take_along_axis(grid, (jnp.arange(top)[None, :] + offset_by) % top, axis=1)


def portions_of(number_of, total, most, lean, full):
    portions = [(1 << 20) // math.isqrt(standing ** lean) + 1 for standing in range(1, number_of + 1)]
    largest = most if full else min(most, max(-(-total // number_of), total * portions[0] // sum(portions)))
    least = 1 if total - largest >= number_of - 1 else 0
    given, rest = [largest] + [least] * (number_of - 1), total - largest - least * (number_of - 1)
    while rest > 0:
        candidates = [i for i in range(1, number_of) if given[i] < largest] or [i for i in range(1, number_of) if given[i] < most]
        whole, budget = sum([portions[i] for i in candidates]), rest
        for i in candidates:
            addition = min(most - given[i], max(1, budget * portions[i] // whole), rest)
            given[i] = given[i] + addition
            rest = rest - addition
    return np.array(given)


def gaussian(rng, dims, deviation, reach, split=(), kind=jnp.bfloat16):
    values = deviation * jax.random.normal(rng, dims, jnp.float32)
    if split:
        values = values * block_scale(rng, dims, split, -0.22, 0.18)
    return jnp.clip(values, -reach, reach).astype(kind)


def setup_inputs(seed: int = 0) -> dict:
    key_of = jax.random.split(jax.random.key(seed), 7)
    tokens = gaussian(key_of[0], (TOKENS, D), 1.0, 6.0, ((0, 32), (1, 24)))
    router_weight = gaussian(key_of[1], (D, EXPERTS), D ** -0.5, 0.078125, ((0, 24),))
    expert_ids_keys = jax.random.split(jax.random.fold_in(key_of[2], 1), TOKENS // TOK_DP)
    expert_ids_turns = jax.random.permutation(jax.random.fold_in(key_of[2], 3), TOKENS // TOK_DP)
    expert_ids = jax.vmap(lambda own, number: assign_block(jax.random.fold_in(key_of[2], 2), own, number, TOK_DP, EXPERTS, 2, CAP, 2))(expert_ids_keys, expert_ids_turns).reshape((TOKENS, 2))
    w_gate = gaussian(key_of[3], (N_DP, D, FF // (N_DP // EXPERTS)), D ** -0.5, 0.078125, ((0, 32), (2, 24)))
    w_up = gaussian(key_of[4], (N_DP, D, FF // (N_DP // EXPERTS)), D ** -0.5, 0.078125, ((0, 32), (2, 24)))
    w_down = gaussian(key_of[5], (N_DP, FF // (N_DP // EXPERTS), D), FF ** -0.5, 0.0546875, ((0, 32), (1, 24)))
    return dict(tokens=tokens, router_weight=router_weight, expert_ids=expert_ids, w_gate=w_gate, w_up=w_up, w_down=w_down)


def expert_block(rows, gate_w, up_w, down_w):
    count = rows.shape[0]
    piece = gate_w.shape[2] // N_TENSOR

    def replica(total, parts):
        g_w, u_w, d_w = parts
        gate = jnp.dot(rows, g_w, preferred_element_type=jnp.float32)
        up = jnp.dot(rows, u_w, preferred_element_type=jnp.float32)
        hidden = (jax.nn.silu(gate) * up).astype(jnp.bfloat16)
        hidden_blocks = hidden.reshape(count, N_TENSOR, piece).transpose(1, 0, 2)
        down_blocks = d_w.reshape(N_TENSOR, piece, D)

        def add_block(acc, pair):
            h_part, d_part = pair
            rounded = lax.optimization_barrier(jnp.dot(h_part, d_part, preferred_element_type=jnp.float32).astype(jnp.bfloat16))
            return acc + rounded.astype(jnp.float32), None

        summed, _ = lax.scan(add_block, jnp.zeros((count, D), jnp.float32), (hidden_blocks, down_blocks))
        share = lax.optimization_barrier(summed.astype(jnp.bfloat16))
        return total + share.astype(jnp.float32), None

    result, _ = lax.scan(replica, jnp.zeros((count, D), jnp.float32), (gate_w, up_w, down_w))
    return result


def reference(tokens, router_weight, expert_ids, w_gate, w_up, w_down):
    groups = N_DP // EXPERTS
    slots_all = N_DP * CAP
    logits = jnp.dot(tokens, router_weight, preferred_element_type=jnp.float32)
    chosen = jnp.take_along_axis(logits, expert_ids.astype(jnp.int32), axis=1)
    first = jax.nn.sigmoid(chosen[:, 0] - chosen[:, 1])
    gates = jnp.stack([first, 1.0 - first], axis=1)
    flat = expert_ids.astype(jnp.int32).reshape(N_DP, TOK_DP * 2)
    onehot = (flat[:, :, None] == jnp.arange(EXPERTS, dtype=jnp.int32)[None, None, :]).astype(jnp.int32)
    ranks = jnp.sum((jnp.cumsum(onehot, axis=1).astype(jnp.int32) - onehot) * onehot, axis=2).astype(jnp.int32)
    blocks = jnp.arange(N_DP, dtype=jnp.int32)[:, None]
    position = (flat * slots_all + blocks * CAP + ranks).astype(jnp.int32).reshape(TOKENS, 2)
    buffers = jnp.zeros((EXPERTS * slots_all, D), jnp.bfloat16)
    buffers = buffers.at[position[:, 0]].set(tokens).at[position[:, 1]].set(tokens)
    buffers = buffers.reshape(EXPERTS, slots_all, D)
    gate_all = w_gate.reshape(EXPERTS, groups, D, -1)
    up_all = w_up.reshape(EXPERTS, groups, D, -1)
    down_all = w_down.reshape(EXPERTS, groups, -1, D)
    outputs = lax.map(lambda parts: expert_block(parts[0], parts[1], parts[2], parts[3]), (buffers, gate_all, up_all, down_all))
    outputs = outputs.reshape(EXPERTS * slots_all, D)
    mixed = gates[:, 0:1] * outputs[position[:, 0]] + gates[:, 1:2] * outputs[position[:, 1]]
    return mixed.astype(jnp.bfloat16)
```

```python
import jax
import jax.numpy as jnp
from jax import lax
from jax.experimental import pallas as pl
from jax.experimental.pallas import tpu as pltpu
from jax.sharding import Mesh
from jax.sharding import PartitionSpec as P


CAP = 12
LANES = 128
CHUNK = 2 * CAP
FAR = ("zh", "yq", "yp", "z")
f32, bf16 = jnp.float32, jnp.bfloat16


def call(body, out_shape, flops, nbytes, **kw):
    return pl.pallas_call(
        body,
        out_shape=out_shape,
        cost_estimate=pl.CostEstimate(flops=flops, bytes_accessed=nbytes, transcendentals=0),
        **kw,
    )


def slot_matrices(ids, experts):
    tok = ids.shape[1]
    which = lax.broadcasted_iota(jnp.int32, (experts, tok), 0)
    chosen = [(which == ids[k : k + 1, :]).astype(f32) for k in range(2)]
    earlier = (
        lax.broadcasted_iota(jnp.int32, (tok, tok), 0) < lax.broadcasted_iota(jnp.int32, (tok, tok), 1)
    ).astype(f32)
    counts = jnp.dot(chosen[0] + chosen[1], earlier, preferred_element_type=f32)
    rows = experts * CHUNK
    flat = lax.broadcasted_iota(jnp.int32, (rows, tok), 0)
    expert = jnp.zeros((rows, tok), jnp.int32)
    for e in range(1, experts):
        expert = expert + (flat >= e * CHUNK).astype(jnp.int32)
    row = flat - expert * CHUNK
    slot = jnp.where(row < 12, row, jnp.where(row < 16, row - 4, row - 16))
    place = expert * CAP + slot
    matrices = []
    for k in range(2):
        rank = jnp.sum(chosen[k] * counts, axis=0, keepdims=True)
        position = ids[k : k + 1, :] * CAP + (rank + 0.5).astype(jnp.int32)
        matrices.append((place == position).astype(f32))
    return chosen, matrices, row < 12


def pack_kernel(ids_ref, tokens_ref, router_ref, out_ref, logits_ref):
    experts, copies = out_ref.shape[0], out_ref.shape[1]
    tok = tokens_ref.shape[0]
    _, (first, second), low = slot_matrices(ids_ref[...], experts)
    placing = first + second
    zero = jnp.zeros_like(placing)
    tokens = tokens_ref[...]
    packed = jnp.dot(
        jnp.where(low, placing, zero).astype(bf16), tokens[:, :LANES], preferred_element_type=f32
    ) + jnp.dot(jnp.where(low, zero, placing).astype(bf16), tokens[:, LANES:], preferred_element_type=f32)
    packed = packed.reshape(experts, CHUNK, LANES).astype(bf16)
    for n in range(copies):
        out_ref[:, n] = packed
    logits = lax.dot_general(router_ref[...], tokens, (((1,), (1,)), ((), ())), preferred_element_type=f32)
    logits_ref[...] = jnp.zeros_like(logits_ref)
    logits_ref[:, :tok] = logits


def spread_kernel(in_ref, lo_ref, hi_ref):
    sources, zs = in_ref.shape[0], in_ref.shape[1]
    top = lax.broadcasted_iota(jnp.int32, (8, LANES), 0) < 4
    for z in range(zs):
        ref, at = (lo_ref, z) if z < zs // 2 else (hi_ref, z - zs // 2)
        for p in range(sources // 2):
            a = in_ref[2 * p, z].astype(f32)
            b = in_ref[2 * p + 1, z].astype(f32)
            ac, bc = a[8:16], b[8:16]
            left = jnp.concatenate([a[0:8], jnp.where(top, ac, pltpu.roll(bc, 4, 0)), b[0:8]], axis=0)
            right = jnp.concatenate([a[16:24], jnp.where(top, pltpu.roll(ac, 4, 0), bc), b[16:24]], axis=0)
            ref[at, CHUNK * p : CHUNK * (p + 1), :LANES] = left.astype(bf16)
            ref[at, CHUNK * p : CHUNK * (p + 1), LANES:] = right.astype(bf16)


def unspread_kernel(*refs):
    ins, out_ref = refs[:-1], refs[-1]
    sources, zs = out_ref.shape[0], out_ref.shape[1]
    top = lax.broadcasted_iota(jnp.int32, (8, LANES), 0) < 4
    for z in range(zs):
        half, at = (0, z) if z < zs // 2 else (1, z - zs // 2)
        for p in range(sources // 2):
            total = None
            for n in range(len(ins) // 2):
                term = ins[2 * n + half][at, CHUNK * p : CHUNK * (p + 1), :].astype(f32)
                total = term if total is None else total + term
            y, w = total[:, :LANES], total[:, LANES:]
            yc, wc = y[8:16], w[8:16]
            a = jnp.concatenate([y[0:8], jnp.where(top, yc, pltpu.roll(wc, 4, 0)), w[0:8]], axis=0)
            b = jnp.concatenate([y[16:24], jnp.where(top, pltpu.roll(yc, 4, 0), wc), w[16:24]], axis=0)
            out_ref[2 * p, z] = a.astype(bf16)
            out_ref[2 * p + 1, z] = b.astype(bf16)


def products(lo_ref, hi_ref, weights, total):
    half = lo_ref.shape[0]
    for z in range(2 * half):
        rows = lo_ref[z] if z < half else hi_ref[z - half]
        both = jnp.concatenate([w[z, 0] for w in weights], axis=1)
        term = jnp.dot(rows, both, preferred_element_type=f32)
        total = term if total is None else total + term
    return total


def gate_up_kernel(more, xi_ref, *refs):
    lo_ref, hi_ref, *weights = refs[:6]
    total = refs[6][...] if more else None
    refs[-1][...] = products(lo_ref, hi_ref, weights, total)


def down(hidden, own_ref, other_ref, column, z, xs):
    at = pl.ds(pl.multiple_of((z * xs + column) * 256, 256), 256)
    both = jnp.concatenate([own_ref[:, at], other_ref[:, at]], axis=0)
    return jnp.dot(hidden, both, preferred_element_type=f32).astype(bf16)


def turn_kernel(xs, xi_ref, *refs):
    lo_ref, hi_ref, *weights = refs[:6]
    total_ref, own_ref, other_ref, hidden_ref, out_lo, out_hi = refs[6:]
    total = products(lo_ref, hi_ref, weights, total_ref[...])
    units = total.shape[1] // 2
    gate, up = total[:, :units], total[:, units:]
    hidden = (jax.nn.silu(gate) * up).astype(bf16)
    hidden_ref[...] = hidden
    half = lo_ref.shape[0]
    for z in range(2 * half):
        value = down(hidden, own_ref, other_ref, xi_ref[0], z, xs)
        if z < half:
            out_lo[z] = value
        else:
            out_hi[z - half] = value


def down_kernel(xs, xi_ref, hidden_ref, own_ref, other_ref, *outs):
    hidden = hidden_ref[...]
    half = outs[0].shape[0]
    for n in range(len(outs) // 2):
        for z in range(2 * half):
            value = down(hidden, own_ref, other_ref, xi_ref[n], z, xs)
            if z < half:
                outs[2 * n][z] = value
            else:
                outs[2 * n + 1][z - half] = value


def merge_kernel(ids_ref, logits_ref, in_ref, out_ref):
    experts, copies = in_ref.shape[0], in_ref.shape[1]
    tok = ids_ref.shape[1]
    chosen, (first, second), low = slot_matrices(ids_ref[...], experts)
    logits = logits_ref[0]
    for n in range(1, logits_ref.shape[0]):
        logits = logits + logits_ref[n]
    logits = logits[:, :tok]
    a = jnp.sum(chosen[0] * logits, axis=0, keepdims=True)
    b = jnp.sum(chosen[1] * logits, axis=0, keepdims=True)
    gate = jax.nn.sigmoid(a - b)
    weights = first * gate + second * (1.0 - gate)
    merged = in_ref[:, 0].astype(f32)
    for n in range(1, copies):
        merged = merged + in_ref[:, n].astype(f32)
    merged = merged.reshape(experts * CHUNK, LANES)
    zero = jnp.zeros_like(weights)
    for h in range(2):
        part = jnp.where(low, weights, zero) if h == 0 else jnp.where(low, zero, weights)
        value = lax.dot_general(
            part, merged, (((0,), (0,)), ((), ())), precision=lax.Precision.HIGHEST, preferred_element_type=f32
        )
        out_ref[:, h * LANES : (h + 1) * LANES] = value.astype(bf16)


def per_device(tokens, router_weight, expert_ids, w_gate, w_up, w_down):
    tok, share = tokens.shape
    xs, zs = lax.axis_size("x"), lax.axis_size("z")
    experts = lax.axis_size(("zh", "yq"))
    sources = experts * 2
    far = sources * zs
    rows = sources * CAP
    half = zs // 2
    assert xs == 4 and share == 256 and zs % 2 == 0
    units = w_gate.shape[2]
    ids = expert_ids.T
    me = lax.axis_index("x")
    near = [((me + k) & (xs - 1)).astype(jnp.int32).reshape(1) for k in (0, 1, 3, 2)]
    forward = [(i, (i + 1) % xs) for i in range(xs)]
    backward = [(i, (i - 1) % xs) for i in range(xs)]

    def ahead(v):
        return lax.ppermute(v, "x", forward)

    def behind(v):
        return lax.ppermute(v, "x", backward)

    messages, logits = call(
        pack_kernel,
        (
            jax.ShapeDtypeStruct((experts, 2 * zs, CHUNK, LANES), bf16),
            jax.ShapeDtypeStruct((experts, LANES), f32),
        ),
        10**7,
        10**6,
        name="pack",
    )(ids, tokens, router_weight.T)
    arrived = lax.all_to_all(messages.reshape(far, CHUNK, LANES), FAR, 0, 0, tiled=True)

    block = jax.ShapeDtypeStruct((half, rows, share), bf16)
    own_lo, own_hi = call(spread_kernel, (block, block), 10**6, 2 * far * CHUNK * LANES * 2, name="spread")(
        arrived.reshape(sources, zs, CHUNK, LANES)
    )

    left_hi = ahead(own_hi)
    right_lo = behind(own_lo)
    left_lo = ahead(own_lo)
    right_hi = behind(own_hi)
    swap = [(0, 1), (1, 0)]
    gate_w, up_w, down_w, _ = lax.optimization_barrier((w_gate[0], w_up[0], w_down[0], own_lo))
    gate_o, up_o, down_o = (lax.ppermute(v, "c", swap) for v in (gate_w, up_w, down_w))
    far_hi = ahead(left_hi)
    far_lo = behind(right_lo)

    stacked = [v.reshape(zs, xs, share, units) for v in (gate_w, gate_o, up_w, up_o)]
    weight_spec = pl.BlockSpec((zs, 1, share, units), lambda g, xi: (0, xi[0], 0, 0))

    def whole(*shape):
        return pl.BlockSpec(shape, lambda g, xi: (0,) * len(shape))

    part = whole(half, rows, share)
    sums = jax.ShapeDtypeStruct((rows, 4 * units), f32)
    sums_spec = whole(rows, 4 * units)
    flops = 2 * rows * zs * share * 4 * units
    nbytes = zs * share * units * 8 + 2 * half * rows * share * 2

    def gate_up(total, column, lo, hi):
        more = total is not None
        return call(
            lambda *refs: gate_up_kernel(more, *refs),
            sums,
            flops,
            nbytes,
            grid_spec=pltpu.PrefetchScalarGridSpec(
                num_scalar_prefetch=1,
                grid=(1,),
                in_specs=[part, part] + [weight_spec] * 4 + [sums_spec] * more,
                out_specs=sums_spec,
            ),
            name="gate_up",
        )(near[column], lo, hi, *stacked, *([total] if more else []))

    total = gate_up(None, 0, own_lo, own_hi)
    total = gate_up(total, 1, right_lo, right_hi)
    total = gate_up(total, 2, left_lo, left_hi)
    down_spec = whole(units, zs * xs * share)
    hidden_spec = whole(rows, 2 * units)
    hidden, opp_lo, opp_hi = call(
        lambda *refs: turn_kernel(xs, *refs),
        (jax.ShapeDtypeStruct((rows, 2 * units), bf16), block, block),
        2 * flops,
        2 * nbytes,
        grid_spec=pltpu.PrefetchScalarGridSpec(
            num_scalar_prefetch=1,
            grid=(1,),
            in_specs=[part, part] + [weight_spec] * 4 + [sums_spec, down_spec, down_spec],
            out_specs=(hidden_spec, part, part),
        ),
        name="turn",
    )(near[3], far_lo, far_hi, *stacked, total, down_w, down_o)

    from_left_lo = ahead(opp_lo)
    from_right_hi = behind(opp_hi)
    outs = call(
        lambda *refs: down_kernel(xs, *refs),
        (block,) * 6,
        2 * flops,
        2 * nbytes,
        grid_spec=pltpu.PrefetchScalarGridSpec(
            num_scalar_prefetch=1,
            grid=(1,),
            in_specs=[hidden_spec, down_spec, down_spec],
            out_specs=(part,) * 6,
        ),
        name="down",
    )(jnp.concatenate([near[1], near[2], near[0]]), hidden, down_w, down_o)
    next_lo, next_hi, prev_lo, prev_hi, mine_lo, mine_hi = outs
    c_hi = ahead(next_hi)
    e_lo = behind(prev_lo)
    c_lo = ahead((next_lo.astype(f32) + from_left_lo.astype(f32)).astype(bf16))
    e_hi = behind((prev_hi.astype(f32) + from_right_hi.astype(f32)).astype(bf16))

    spread_logits, _ = lax.optimization_barrier((logits, mine_lo))
    spread_logits = jnp.broadcast_to(spread_logits[None], (zs * xs, experts, LANES))
    partial_logits = lax.all_to_all(spread_logits, ("z", "x"), 0, 0, tiled=True)

    leaving = call(
        unspread_kernel,
        jax.ShapeDtypeStruct((sources, zs, CHUNK, LANES), bf16),
        10**7,
        4 * far * CHUNK * LANES * 2,
        name="unspread",
    )(mine_lo, mine_hi, c_lo, c_hi, e_lo, e_hi)
    back = lax.all_to_all(leaving.reshape(far, CHUNK, LANES), FAR, 0, 0, tiled=True)
    return call(
        merge_kernel,
        jax.ShapeDtypeStruct((tok, share), bf16),
        10**7,
        10**6,
        name="merge",
    )(ids, partial_logits, back.reshape(experts, 2 * zs, CHUNK, LANES))


def solution(mesh):
    finer = Mesh(mesh.devices.reshape(2, 4, 2, 2, 6, 4), ("zh", "yq", "yp", "c", "z", "x"))
    dp, tensor = ("zh", "yq", "yp", "c"), ("z", "x")
    return jax.shard_map(
        per_device,
        mesh=finer,
        in_specs=(
            P(dp, tensor),
            P(tensor, None),
            P(dp, None),
            P(dp, None, tensor),
            P(dp, None, tensor),
            P(dp, tensor, None),
        ),
        out_specs=P(dp, tensor),
        check_vma=False,
    )
```

```python
import jax
import jax.numpy as jnp
from jax import lax
from jax.experimental import pallas as pl
from jax.experimental.pallas import tpu as pltpu
from jax.sharding import Mesh
from jax.sharding import PartitionSpec as P


CAP = 12
LANES = 128
CHUNK = 2 * CAP
FAR = ("zh", "yq", "yp", "z")
f32, bf16 = jnp.float32, jnp.bfloat16


def call(body, out_shape, flops, nbytes, **kw):
    return pl.pallas_call(
        body,
        out_shape=out_shape,
        cost_estimate=pl.CostEstimate(flops=flops, bytes_accessed=nbytes, transcendentals=0),
        **kw,
    )


def slot_matrices(ids, experts):
    tok = ids.shape[1]
    which = lax.broadcasted_iota(jnp.int32, (experts, tok), 0)
    chosen = [(which == ids[k : k + 1, :]).astype(f32) for k in range(2)]
    earlier = (
        lax.broadcasted_iota(jnp.int32, (tok, tok), 0) < lax.broadcasted_iota(jnp.int32, (tok, tok), 1)
    ).astype(f32)
    counts = jnp.dot(chosen[0] + chosen[1], earlier, preferred_element_type=f32)
    rows = experts * CHUNK
    flat = lax.broadcasted_iota(jnp.int32, (rows, tok), 0)
    expert = jnp.zeros((rows, tok), jnp.int32)
    for e in range(1, experts):
        expert = expert + (flat >= e * CHUNK).astype(jnp.int32)
    row = flat - expert * CHUNK
    slot = jnp.where(row < 12, row, jnp.where(row < 16, row - 4, row - 16))
    place = expert * CAP + slot
    matrices = []
    for k in range(2):
        rank = jnp.sum(chosen[k] * counts, axis=0, keepdims=True)
        position = ids[k : k + 1, :] * CAP + (rank + 0.5).astype(jnp.int32)
        matrices.append((place == position).astype(f32))
    return chosen, matrices, row < 12


def pack_kernel(ids_ref, tokens_ref, router_ref, out_ref, logits_ref):
    experts, copies = out_ref.shape[0], out_ref.shape[1]
    tok = tokens_ref.shape[0]
    _, (first, second), low = slot_matrices(ids_ref[...], experts)
    placing = first + second
    zero = jnp.zeros_like(placing)
    tokens = tokens_ref[...]
    packed = jnp.dot(
        jnp.where(low, placing, zero).astype(bf16), tokens[:, :LANES], preferred_element_type=f32
    ) + jnp.dot(jnp.where(low, zero, placing).astype(bf16), tokens[:, LANES:], preferred_element_type=f32)
    packed = packed.reshape(experts, CHUNK, LANES).astype(bf16)
    for n in range(copies):
        out_ref[:, n] = packed
    logits = lax.dot_general(router_ref[...], tokens, (((1,), (1,)), ((), ())), preferred_element_type=f32)
    each = LANES // tok
    lines = [jnp.concatenate([logits[i + k : i + k + 1] for k in range(each)], axis=1) for i in range(0, experts, each)]
    lines = jnp.concatenate(lines, axis=0)
    for n in range(logits_ref.shape[0]):
        logits_ref[n] = lines


def spread_kernel(in_ref, lo_ref, hi_ref):
    sources, zs = in_ref.shape[0], in_ref.shape[1]
    top = lax.broadcasted_iota(jnp.int32, (8, LANES), 0) < 4
    for z in range(zs):
        ref, at = (lo_ref, z) if z < zs // 2 else (hi_ref, z - zs // 2)
        for p in range(sources // 2):
            a = in_ref[2 * p, z].astype(f32)
            b = in_ref[2 * p + 1, z].astype(f32)
            ac, bc = a[8:16], b[8:16]
            left = jnp.concatenate([a[0:8], jnp.where(top, ac, pltpu.roll(bc, 4, 0)), b[0:8]], axis=0)
            right = jnp.concatenate([a[16:24], jnp.where(top, pltpu.roll(ac, 4, 0), bc), b[16:24]], axis=0)
            ref[at, CHUNK * p : CHUNK * (p + 1), :LANES] = left.astype(bf16)
            ref[at, CHUNK * p : CHUNK * (p + 1), LANES:] = right.astype(bf16)


def unspread_kernel(*refs):
    ins, out_ref = refs[:-1], refs[-1]
    sources, zs = out_ref.shape[0], out_ref.shape[1]
    top = lax.broadcasted_iota(jnp.int32, (8, LANES), 0) < 4
    for z in range(zs):
        half, at = (0, z) if z < zs // 2 else (1, z - zs // 2)
        for p in range(sources // 2):
            total = None
            for n in range(len(ins) // 2):
                term = ins[2 * n + half][at, CHUNK * p : CHUNK * (p + 1), :].astype(f32)
                total = term if total is None else total + term
            y, w = total[:, :LANES], total[:, LANES:]
            yc, wc = y[8:16], w[8:16]
            a = jnp.concatenate([y[0:8], jnp.where(top, yc, pltpu.roll(wc, 4, 0)), w[0:8]], axis=0)
            b = jnp.concatenate([y[16:24], jnp.where(top, pltpu.roll(yc, 4, 0), wc), w[16:24]], axis=0)
            out_ref[2 * p, z] = a.astype(bf16)
            out_ref[2 * p + 1, z] = b.astype(bf16)


def products(lo_ref, hi_ref, weights, total):
    half = lo_ref.shape[0]
    for z in range(2 * half):
        rows = lo_ref[z] if z < half else hi_ref[z - half]
        both = jnp.concatenate([w[z, 0] for w in weights], axis=1)
        term = jnp.dot(rows, both, preferred_element_type=f32)
        total = term if total is None else total + term
    return total


def gate_up_kernel(more, xi_ref, *refs):
    lo_ref, hi_ref, *weights = refs[:6]
    total = refs[6][...] if more else None
    refs[-1][...] = products(lo_ref, hi_ref, weights, total)


def down(hidden, own_ref, other_ref, column, z, xs):
    at = pl.ds(pl.multiple_of((z * xs + column) * 256, 256), 256)
    both = jnp.concatenate([own_ref[:, at], other_ref[:, at]], axis=0)
    return jnp.dot(hidden, both, preferred_element_type=f32).astype(bf16)


def turn_kernel(xs, xi_ref, *refs):
    lo_ref, hi_ref, *weights = refs[:6]
    total_ref, own_ref, other_ref, hidden_ref, out_lo, out_hi = refs[6:]
    total = products(lo_ref, hi_ref, weights, total_ref[...])
    units = total.shape[1] // 2
    gate, up = total[:, :units], total[:, units:]
    hidden = (jax.nn.silu(gate) * up).astype(bf16)
    hidden_ref[...] = hidden
    half = lo_ref.shape[0]
    for z in range(2 * half):
        value = down(hidden, own_ref, other_ref, xi_ref[0], z, xs)
        if z < half:
            out_lo[z] = value
        else:
            out_hi[z - half] = value


def down_kernel(xs, first_ref, second_ref, third_ref, hidden_ref, own_ref, other_ref, *outs):
    hidden = hidden_ref[...]
    half = outs[0].shape[0]
    for n in range(len(outs) // 2):
        for z in range(2 * half):
            value = down(hidden, own_ref, other_ref, (first_ref, second_ref, third_ref)[n][0], z, xs)
            if z < half:
                outs[2 * n][z] = value
            else:
                outs[2 * n + 1][z - half] = value


def merge_kernel(ids_ref, logits_ref, in_ref, out_ref):
    experts, copies = in_ref.shape[0], in_ref.shape[1]
    tok = ids_ref.shape[1]
    chosen, (first, second), low = slot_matrices(ids_ref[...], experts)
    logits = logits_ref[0]
    for n in range(1, logits_ref.shape[0]):
        logits = logits + logits_ref[n]
    logits = jnp.concatenate(
        [logits[i : i + 1, k : k + tok] for i in range(logits.shape[0]) for k in range(0, LANES, tok)], axis=0
    )
    a = jnp.sum(chosen[0] * logits, axis=0, keepdims=True)
    b = jnp.sum(chosen[1] * logits, axis=0, keepdims=True)
    gate = jax.nn.sigmoid(a - b)
    weights = first * gate + second * (1.0 - gate)
    merged = in_ref[:, 0].astype(f32)
    for n in range(1, copies):
        merged = merged + in_ref[:, n].astype(f32)
    merged = merged.reshape(experts * CHUNK, LANES)
    zero = jnp.zeros_like(weights)
    for h in range(2):
        part = jnp.where(low, weights, zero) if h == 0 else jnp.where(low, zero, weights)
        value = lax.dot_general(
            part, merged, (((0,), (0,)), ((), ())), precision=lax.Precision.HIGHEST, preferred_element_type=f32
        )
        out_ref[:, h * LANES : (h + 1) * LANES] = value.astype(bf16)


def block(tokens, router_weight, expert_ids, w_gate, w_up, w_down):
    tok, share = tokens.shape
    xs, zs = lax.axis_size("x"), lax.axis_size("z")
    experts = lax.axis_size(("zh", "yq"))
    sources = experts * 2
    far = sources * zs
    rows = sources * CAP
    half = zs // 2
    assert xs == 4 and share == 256 and zs % 2 == 0
    units = w_gate.shape[2]
    ids = expert_ids.T
    me = lax.axis_index("x")
    near = [((me + k) & (xs - 1)).astype(jnp.int32).reshape(1) for k in (0, 1, 3, 2)]
    forward = [(i, (i + 1) % xs) for i in range(xs)]
    backward = [(i, (i - 1) % xs) for i in range(xs)]

    def ahead(v):
        return lax.ppermute(v, "x", forward)

    def behind(v):
        return lax.ppermute(v, "x", backward)

    messages, logits = call(
        pack_kernel,
        (
            jax.ShapeDtypeStruct((experts, 2 * zs, CHUNK, LANES), bf16),
            jax.ShapeDtypeStruct((zs * xs, experts * tok // LANES, LANES), f32),
        ),
        10**7,
        10**6,
        name="pack",
    )(ids, tokens, router_weight.T)
    partial_logits = lax.all_to_all(logits, ("z", "x"), 0, 0, tiled=True)
    arrived = lax.all_to_all(messages.reshape(far, CHUNK, LANES), FAR, 0, 0, tiled=True)

    part_shape = jax.ShapeDtypeStruct((half, rows, share), bf16)
    own_lo, own_hi = call(spread_kernel, (part_shape, part_shape), 10**6, 2 * far * CHUNK * LANES * 2, name="spread")(
        arrived.reshape(sources, zs, CHUNK, LANES)
    )

    left_hi = ahead(own_hi)
    right_lo = behind(own_lo)
    left_lo = ahead(own_lo)
    right_hi = behind(own_hi)
    swap = [(0, 1), (1, 0)]
    gate_w, up_w, down_w, _ = lax.optimization_barrier((w_gate[0], w_up[0], w_down[0], own_lo))
    gate_o = lax.ppermute(gate_w, "c", swap)
    up_o = lax.ppermute(up_w, "c", swap)
    down_o = lax.ppermute(down_w, "c", swap)
    far_hi = ahead(left_hi)
    far_lo = behind(right_lo)

    stacked = [v.reshape(zs, xs, share, units) for v in (gate_w, gate_o, up_w, up_o)]
    weight_spec = pl.BlockSpec((zs, 1, share, units), lambda g, xi: (0, xi[0], 0, 0))

    def whole(*shape):
        return pl.BlockSpec(shape, lambda g, *xi: (0,) * len(shape))

    part = whole(half, rows, share)
    sums = jax.ShapeDtypeStruct((rows, 4 * units), f32)
    sums_spec = whole(rows, 4 * units)
    flops = 2 * rows * zs * share * 4 * units
    nbytes = zs * share * units * 8 + 2 * half * rows * share * 2

    def gate_up(total, column, lo, hi):
        more = total is not None
        return call(
            lambda *refs: gate_up_kernel(more, *refs),
            sums,
            flops,
            nbytes,
            grid_spec=pltpu.PrefetchScalarGridSpec(
                num_scalar_prefetch=1,
                grid=(1,),
                in_specs=[part, part] + [weight_spec] * 4 + [sums_spec] * more,
                out_specs=sums_spec,
            ),
            name="gate_up",
        )(near[column], lo, hi, *stacked, *([total] if more else []))

    total = gate_up(None, 0, own_lo, own_hi)
    total = gate_up(total, 1, right_lo, right_hi)
    total = gate_up(total, 2, left_lo, left_hi)
    down_spec = whole(units, zs * xs * share)
    hidden_spec = whole(rows, 2 * units)
    hidden, opp_lo, opp_hi = call(
        lambda *refs: turn_kernel(xs, *refs),
        (jax.ShapeDtypeStruct((rows, 2 * units), bf16), part_shape, part_shape),
        2 * flops,
        2 * nbytes,
        grid_spec=pltpu.PrefetchScalarGridSpec(
            num_scalar_prefetch=1,
            grid=(1,),
            in_specs=[part, part] + [weight_spec] * 4 + [sums_spec, down_spec, down_spec],
            out_specs=(hidden_spec, part, part),
        ),
        name="turn",
    )(near[3], far_lo, far_hi, *stacked, total, down_w, down_o)

    from_left_lo = ahead(opp_lo)
    from_right_hi = behind(opp_hi)
    outs = call(
        lambda *refs: down_kernel(xs, *refs),
        (part_shape,) * 6,
        2 * flops,
        2 * nbytes,
        grid_spec=pltpu.PrefetchScalarGridSpec(
            num_scalar_prefetch=3,
            grid=(1,),
            in_specs=[hidden_spec, down_spec, down_spec],
            out_specs=(part,) * 6,
        ),
        name="down",
    )(near[1], near[2], near[0], hidden, down_w, down_o)
    next_lo, next_hi, prev_lo, prev_hi, mine_lo, mine_hi = outs
    c_hi = ahead(next_hi)
    e_lo = behind(prev_lo)
    c_lo = ahead((next_lo.astype(f32) + from_left_lo.astype(f32)).astype(bf16))
    e_hi = behind((prev_hi.astype(f32) + from_right_hi.astype(f32)).astype(bf16))

    leaving = call(
        unspread_kernel,
        jax.ShapeDtypeStruct((sources, zs, CHUNK, LANES), bf16),
        10**7,
        4 * far * CHUNK * LANES * 2,
        name="unspread",
    )(mine_lo, mine_hi, c_lo, c_hi, e_lo, e_hi)
    back = lax.all_to_all(leaving.reshape(far, CHUNK, LANES), FAR, 0, 0, tiled=True)
    return call(
        merge_kernel,
        jax.ShapeDtypeStruct((tok, share), bf16),
        10**7,
        10**6,
        name="merge",
    )(ids, partial_logits, back.reshape(experts, 2 * zs, CHUNK, LANES))


def solution(mesh):
    finer = Mesh(mesh.devices.reshape(2, 4, 2, 2, 6, 4), ("zh", "yq", "yp", "c", "z", "x"))
    dp, tensor = ("zh", "yq", "yp", "c"), ("z", "x")
    return jax.shard_map(
        block,
        mesh=finer,
        in_specs=(
            P(dp, tensor),
            P(tensor, None),
            P(dp, None),
            P(dp, None, tensor),
            P(dp, None, tensor),
            P(dp, tensor, None),
        ),
        out_specs=P(dp, tensor),
        check_vma=False,
    )
```

```python
import jax
import jax.numpy as jnp
from jax import lax
from jax.experimental import pallas as pl
from jax.experimental.pallas import tpu as pltpu
from jax.sharding import Mesh
from jax.sharding import PartitionSpec as P


CAP = 12
LANES = 128
CHUNK = 2 * CAP
FAR = ("zh", "yq", "yp", "z")
f32, bf16 = jnp.float32, jnp.bfloat16


def call(body, out_shape, flops, nbytes, mib=8, **kw):
    return pl.pallas_call(
        body,
        compiler_params=pltpu.CompilerParams(vmem_limit_bytes=mib * 2**20),
        out_shape=out_shape,
        cost_estimate=pl.CostEstimate(flops=flops, bytes_accessed=nbytes, transcendentals=0),
        **kw,
    )


def slot_matrices(ids, experts):
    tok = ids.shape[1]
    which = lax.broadcasted_iota(jnp.int32, (experts, tok), 0)
    chosen = [(which == ids[k : k + 1, :]).astype(f32) for k in range(2)]
    earlier = (
        lax.broadcasted_iota(jnp.int32, (tok, tok), 0) < lax.broadcasted_iota(jnp.int32, (tok, tok), 1)
    ).astype(f32)
    counts = jnp.dot(chosen[0] + chosen[1], earlier, preferred_element_type=f32)
    rows = experts * CHUNK
    flat = lax.broadcasted_iota(jnp.int32, (rows, tok), 0)
    expert = jnp.zeros((rows, tok), jnp.int32)
    for e in range(1, experts):
        expert = expert + (flat >= e * CHUNK).astype(jnp.int32)
    row = flat - expert * CHUNK
    slot = jnp.where(row < 12, row, jnp.where(row < 16, row - 4, row - 16))
    place = expert * CAP + slot
    matrices = []
    for k in range(2):
        rank = jnp.sum(chosen[k] * counts, axis=0, keepdims=True)
        position = ids[k : k + 1, :] * CAP + (rank + 0.5).astype(jnp.int32)
        matrices.append((place == position).astype(f32))
    return chosen, matrices, row < 12


def pack_kernel(ids_ref, tokens_ref, router_ref, out_ref, logits_ref):
    experts, copies = out_ref.shape[0], out_ref.shape[1]
    tok = tokens_ref.shape[0]
    _, (first, second), low = slot_matrices(ids_ref[...], experts)
    placing = first + second
    zero = jnp.zeros_like(placing)
    tokens = tokens_ref[...]
    packed = jnp.dot(
        jnp.where(low, placing, zero).astype(bf16), tokens[:, :LANES], preferred_element_type=f32
    ) + jnp.dot(jnp.where(low, zero, placing).astype(bf16), tokens[:, LANES:], preferred_element_type=f32)
    packed = packed.reshape(experts, CHUNK, LANES).astype(bf16)
    for n in range(copies):
        out_ref[:, n] = packed
    logits = lax.dot_general(router_ref[...], tokens, (((1,), (1,)), ((), ())), preferred_element_type=f32)
    each = LANES // tok
    lines = [jnp.concatenate([logits[i + k : i + k + 1] for k in range(each)], axis=1) for i in range(0, experts, each)]
    lines = jnp.concatenate(lines, axis=0)
    for n in range(logits_ref.shape[0]):
        logits_ref[n] = lines


def spread_kernel(in_ref, lo_ref, hi_ref):
    sources, zs = in_ref.shape[0], in_ref.shape[1]
    top = lax.broadcasted_iota(jnp.int32, (8, LANES), 0) < 4
    for z in range(zs):
        ref, at = (lo_ref, z) if z < zs // 2 else (hi_ref, z - zs // 2)
        for p in range(sources // 2):
            a = in_ref[2 * p, z].astype(f32)
            b = in_ref[2 * p + 1, z].astype(f32)
            ac, bc = a[8:16], b[8:16]
            left = jnp.concatenate([a[0:8], jnp.where(top, ac, pltpu.roll(bc, 4, 0)), b[0:8]], axis=0)
            right = jnp.concatenate([a[16:24], jnp.where(top, pltpu.roll(ac, 4, 0), bc), b[16:24]], axis=0)
            ref[at, CHUNK * p : CHUNK * (p + 1), :LANES] = left.astype(bf16)
            ref[at, CHUNK * p : CHUNK * (p + 1), LANES:] = right.astype(bf16)


def unspread_kernel(*refs):
    ins, out_ref = refs[:-1], refs[-1]
    sources, zs = out_ref.shape[0], out_ref.shape[1]
    top = lax.broadcasted_iota(jnp.int32, (8, LANES), 0) < 4
    for z in range(zs):
        half, at = (0, z) if z < zs // 2 else (1, z - zs // 2)
        for p in range(sources // 2):
            total = None
            for n in range(len(ins) // 2):
                term = ins[2 * n + half][at, CHUNK * p : CHUNK * (p + 1), :].astype(f32)
                total = term if total is None else total + term
            y, w = total[:, :LANES], total[:, LANES:]
            yc, wc = y[8:16], w[8:16]
            a = jnp.concatenate([y[0:8], jnp.where(top, yc, pltpu.roll(wc, 4, 0)), w[0:8]], axis=0)
            b = jnp.concatenate([y[16:24], jnp.where(top, pltpu.roll(yc, 4, 0), wc), w[16:24]], axis=0)
            out_ref[2 * p, z] = a.astype(bf16)
            out_ref[2 * p + 1, z] = b.astype(bf16)


def down(hidden, own_ref, other_ref, column, z, xs):
    at = pl.ds(pl.multiple_of((z * xs + column) * 256, 256), 256)
    both = jnp.concatenate([own_ref[:, at], other_ref[:, at]], axis=0)
    return jnp.dot(hidden, both, preferred_element_type=f32).astype(bf16)


def turn_kernel(xs, near_ref, *refs):
    parts, weights = refs[: 2 * xs], refs[2 * xs : 2 * xs + 4]
    own_ref, other_ref, hidden_ref, out_lo, out_hi = refs[2 * xs + 4 :]
    half, _, share = parts[0].shape
    total = None
    for n in range(xs):
        for z in range(2 * half):
            rows = parts[2 * n + z // half][z % half]
            at = pl.ds(pl.multiple_of((z * xs + near_ref[n]) * share, share), share)
            both = jnp.concatenate([w[at, :] for w in weights], axis=1)
            term = jnp.dot(rows, both, preferred_element_type=f32)
            total = term if total is None else total + term
    units = total.shape[1] // 2
    gate, up = total[:, :units], total[:, units:]
    hidden = (jax.nn.silu(gate) * up).astype(bf16)
    hidden_ref[...] = hidden
    for z in range(2 * half):
        value = down(hidden, own_ref, other_ref, near_ref[xs - 1], z, xs)
        if z < half:
            out_lo[z] = value
        else:
            out_hi[z - half] = value


def down_kernel(xs, near_ref, hidden_ref, own_ref, other_ref, *outs):
    hidden = hidden_ref[...]
    half = outs[0].shape[0]
    for n, place in enumerate((1, 2, 0)):
        for z in range(2 * half):
            value = down(hidden, own_ref, other_ref, near_ref[place], z, xs)
            if z < half:
                outs[2 * n][z] = value
            else:
                outs[2 * n + 1][z - half] = value


def merge_kernel(ids_ref, logits_ref, in_ref, out_ref):
    experts, copies = in_ref.shape[0], in_ref.shape[1]
    tok = ids_ref.shape[1]
    chosen, (first, second), low = slot_matrices(ids_ref[...], experts)
    logits = logits_ref[0]
    for n in range(1, logits_ref.shape[0]):
        logits = logits + logits_ref[n]
    logits = jnp.concatenate(
        [logits[i : i + 1, k : k + tok] for i in range(logits.shape[0]) for k in range(0, LANES, tok)], axis=0
    )
    a = jnp.sum(chosen[0] * logits, axis=0, keepdims=True)
    b = jnp.sum(chosen[1] * logits, axis=0, keepdims=True)
    gate = jax.nn.sigmoid(a - b)
    weights = first * gate + second * (1.0 - gate)
    merged = in_ref[:, 0].astype(f32)
    for n in range(1, copies):
        merged = merged + in_ref[:, n].astype(f32)
    merged = merged.reshape(experts * CHUNK, LANES)
    zero = jnp.zeros_like(weights)
    for h in range(2):
        part = jnp.where(low, weights, zero) if h == 0 else jnp.where(low, zero, weights)
        value = lax.dot_general(
            part, merged, (((0,), (0,)), ((), ())), precision=lax.Precision.HIGHEST, preferred_element_type=f32
        )
        out_ref[:, h * LANES : (h + 1) * LANES] = value.astype(bf16)


def block(tokens, router_weight, expert_ids, w_gate, w_up, w_down):
    tok, share = tokens.shape
    xs, zs = lax.axis_size("x"), lax.axis_size("z")
    experts = lax.axis_size(("zh", "yq"))
    sources = experts * 2
    far = sources * zs
    rows = sources * CAP
    half = zs // 2
    assert xs == 4 and share == 256 and zs % 2 == 0
    units = w_gate.shape[2]
    ids = expert_ids.T
    me = lax.axis_index("x")
    near = ((me + jnp.array([0, 1, 3, 2], jnp.int32)) & (xs - 1)).astype(jnp.int32)
    forward = [(i, (i + 1) % xs) for i in range(xs)]
    backward = [(i, (i - 1) % xs) for i in range(xs)]

    def ahead(v):
        return lax.ppermute(v, "x", forward)

    def behind(v):
        return lax.ppermute(v, "x", backward)

    messages, logits = call(
        pack_kernel,
        (
            jax.ShapeDtypeStruct((experts, 2 * zs, CHUNK, LANES), bf16),
            jax.ShapeDtypeStruct((zs * xs, experts * tok // LANES, LANES), f32),
        ),
        10**7,
        10**6,
        name="pack",
    )(ids, tokens, router_weight.T)
    partial_logits = lax.all_to_all(logits, ("z", "x"), 0, 0, tiled=True)
    arrived = lax.all_to_all(messages.reshape(far, CHUNK, LANES), FAR, 0, 0, tiled=True)

    part_shape = jax.ShapeDtypeStruct((half, rows, share), bf16)
    own_lo, own_hi = call(spread_kernel, (part_shape, part_shape), 10**6, 2 * far * CHUNK * LANES * 2, name="spread")(
        arrived.reshape(sources, zs, CHUNK, LANES)
    )

    left_hi = ahead(own_hi)
    right_lo = behind(own_lo)
    left_lo = ahead(own_lo)
    right_hi = behind(own_hi)
    swap = [(0, 1), (1, 0)]
    gate_w, up_w, down_w, _ = lax.optimization_barrier((w_gate[0], w_up[0], w_down[0], own_lo))
    gate_o = lax.ppermute(gate_w, "c", swap)
    up_o = lax.ppermute(up_w, "c", swap)
    down_o = lax.ppermute(down_w, "c", swap)
    far_hi = ahead(left_hi)
    far_lo = behind(right_lo)

    smem = pl.BlockSpec(memory_space=pltpu.SMEM)
    vmem = pl.BlockSpec(memory_space=pltpu.VMEM)
    flops = 2 * rows * zs * xs * share * 4 * units
    nbytes = zs * xs * share * units * 8 + 2 * xs * half * rows * share * 2
    hidden, opp_lo, opp_hi = call(
        lambda *refs: turn_kernel(xs, *refs),
        (jax.ShapeDtypeStruct((rows, 2 * units), bf16), part_shape, part_shape),
        flops,
        nbytes,
        mib=24,
        in_specs=[smem] + [vmem] * (2 * xs + 6),
        name="turn",
    )(
        near,
        own_lo,
        own_hi,
        right_lo,
        right_hi,
        left_lo,
        left_hi,
        far_lo,
        far_hi,
        gate_w,
        gate_o,
        up_w,
        up_o,
        down_w,
        down_o,
    )

    from_left_lo = ahead(opp_lo)
    from_right_hi = behind(opp_hi)
    outs = call(
        lambda *refs: down_kernel(xs, *refs),
        (part_shape,) * 6,
        flops // 2,
        nbytes // 2,
        mib=12,
        in_specs=[smem] + [vmem] * 3,
        name="down",
    )(near, hidden, down_w, down_o)
    next_lo, next_hi, prev_lo, prev_hi, mine_lo, mine_hi = outs
    c_hi = ahead(next_hi)
    e_lo = behind(prev_lo)
    c_lo = ahead((next_lo.astype(f32) + from_left_lo.astype(f32)).astype(bf16))
    e_hi = behind((prev_hi.astype(f32) + from_right_hi.astype(f32)).astype(bf16))

    leaving = call(
        unspread_kernel,
        jax.ShapeDtypeStruct((sources, zs, CHUNK, LANES), bf16),
        10**7,
        4 * far * CHUNK * LANES * 2,
        name="unspread",
    )(mine_lo, mine_hi, c_lo, c_hi, e_lo, e_hi)
    back = lax.all_to_all(leaving.reshape(far, CHUNK, LANES), FAR, 0, 0, tiled=True)
    return call(
        merge_kernel,
        jax.ShapeDtypeStruct((tok, share), bf16),
        10**7,
        10**6,
        name="merge",
    )(ids, partial_logits, back.reshape(experts, 2 * zs, CHUNK, LANES))


def solution(mesh):
    finer = Mesh(mesh.devices.reshape(2, 4, 2, 2, 6, 4), ("zh", "yq", "yp", "c", "z", "x"))
    dp, tensor = ("zh", "yq", "yp", "c"), ("z", "x")
    return jax.shard_map(
        block,
        mesh=finer,
        in_specs=(
            P(dp, tensor),
            P(tensor, None),
            P(dp, None),
            P(dp, None, tensor),
            P(dp, None, tensor),
            P(dp, tensor, None),
        ),
        out_specs=P(dp, tensor),
        check_vma=False,
    )
```

```python
import jax
import jax.numpy as jnp
from jax import lax
from jax.experimental import pallas as pl
from jax.experimental.pallas import tpu as pltpu
from jax.sharding import Mesh
from jax.sharding import PartitionSpec as P


CAP = 12
LANES = 128
CHUNK = 2 * CAP
FAR = ("zh", "yq", "yp", "z")
f32, bf16 = jnp.float32, jnp.bfloat16


def call(body, out_shape, flops, nbytes, mib=8, **kw):
    return pl.pallas_call(
        body,
        compiler_params=pltpu.CompilerParams(vmem_limit_bytes=mib * 2**20),
        out_shape=out_shape,
        cost_estimate=pl.CostEstimate(flops=flops, bytes_accessed=nbytes, transcendentals=0),
        **kw,
    )


def slot_matrices(ids, experts):
    tok = ids.shape[1]
    which = lax.broadcasted_iota(jnp.int32, (experts, tok), 0)
    chosen = [(which == ids[k : k + 1, :]).astype(f32) for k in range(2)]
    earlier = (
        lax.broadcasted_iota(jnp.int32, (tok, tok), 0) < lax.broadcasted_iota(jnp.int32, (tok, tok), 1)
    ).astype(f32)
    counts = jnp.dot(chosen[0] + chosen[1], earlier, preferred_element_type=f32)
    rows = experts * CHUNK
    flat = lax.broadcasted_iota(jnp.int32, (rows, tok), 0)
    expert = jnp.zeros((rows, tok), jnp.int32)
    for e in range(1, experts):
        expert = expert + (flat >= e * CHUNK).astype(jnp.int32)
    row = flat - expert * CHUNK
    slot = jnp.where(row < 12, row, jnp.where(row < 16, row - 4, row - 16))
    place = expert * CAP + slot
    matrices = []
    for k in range(2):
        rank = jnp.sum(chosen[k] * counts, axis=0, keepdims=True)
        position = ids[k : k + 1, :] * CAP + (rank + 0.5).astype(jnp.int32)
        matrices.append((place == position).astype(f32))
    return chosen, matrices, row < 12


def pack_kernel(ids_ref, tokens_ref, router_ref, out_ref, logits_ref):
    experts, copies = out_ref.shape[0], out_ref.shape[1]
    tok = tokens_ref.shape[0]
    _, (first, second), low = slot_matrices(ids_ref[...], experts)
    placing = first + second
    zero = jnp.zeros_like(placing)
    tokens = tokens_ref[...]
    packed = jnp.dot(
        jnp.where(low, placing, zero).astype(bf16), tokens[:, :LANES], preferred_element_type=f32
    ) + jnp.dot(jnp.where(low, zero, placing).astype(bf16), tokens[:, LANES:], preferred_element_type=f32)
    packed = packed.reshape(experts, CHUNK, LANES).astype(bf16)
    for n in range(copies):
        out_ref[:, n] = packed
    logits = lax.dot_general(router_ref[...], tokens, (((1,), (1,)), ((), ())), preferred_element_type=f32)
    each = LANES // tok
    lines = [jnp.concatenate([logits[i + k : i + k + 1] for k in range(each)], axis=1) for i in range(0, experts, each)]
    lines = jnp.concatenate(lines, axis=0)
    for n in range(logits_ref.shape[0]):
        logits_ref[n] = lines


def spread_kernel(in_ref, out_ref):
    sources, zs = in_ref.shape[0], in_ref.shape[1]
    top = lax.broadcasted_iota(jnp.int32, (8, LANES), 0) < 4
    for z in range(zs):
        for p in range(sources // 2):
            a = in_ref[2 * p, z].astype(f32)
            b = in_ref[2 * p + 1, z].astype(f32)
            ac, bc = a[8:16], b[8:16]
            left = jnp.concatenate([a[0:8], jnp.where(top, ac, pltpu.roll(bc, 4, 0)), b[0:8]], axis=0)
            right = jnp.concatenate([a[16:24], jnp.where(top, pltpu.roll(ac, 4, 0), bc), b[16:24]], axis=0)
            out_ref[z, CHUNK * p : CHUNK * (p + 1), :LANES] = left.astype(bf16)
            out_ref[z, CHUNK * p : CHUNK * (p + 1), LANES:] = right.astype(bf16)


def unspread_kernel(*refs):
    ins, out_ref = refs[:-1], refs[-1]
    sources, zs = out_ref.shape[0], out_ref.shape[1]
    top = lax.broadcasted_iota(jnp.int32, (8, LANES), 0) < 4
    for z in range(zs):
        for p in range(sources // 2):
            total = None
            for ref in ins:
                term = ref[z, CHUNK * p : CHUNK * (p + 1), :].astype(f32)
                total = term if total is None else total + term
            y, w = total[:, :LANES], total[:, LANES:]
            yc, wc = y[8:16], w[8:16]
            a = jnp.concatenate([y[0:8], jnp.where(top, yc, pltpu.roll(wc, 4, 0)), w[0:8]], axis=0)
            b = jnp.concatenate([y[16:24], jnp.where(top, pltpu.roll(yc, 4, 0), wc), w[16:24]], axis=0)
            out_ref[2 * p, z] = a.astype(bf16)
            out_ref[2 * p + 1, z] = b.astype(bf16)


def products(blocks, columns, weights, total):
    xs = 4
    for block, column in zip(blocks, columns):
        for z, rows in enumerate(block):
            share = rows.shape[1]
            at = pl.ds(pl.multiple_of((z * xs + column) * share, share), share)
            both = jnp.concatenate([w[at, :] for w in weights], axis=1)
            term = jnp.dot(rows, both, preferred_element_type=f32)
            total = term if total is None else total + term
    return total


def gate_up_kernel(places, near_ref, *refs):
    parts, weights, more = refs[: len(places)], refs[len(places) : len(places) + 4], refs[len(places) + 4 : -1]
    blocks = [[p[z] for z in range(p.shape[0])] for p in parts]
    refs[-1][...] = products(blocks, [near_ref[n] for n in places], weights, more[0][...] if more else None)


def down(hidden, own_ref, other_ref, column, z, xs):
    at = pl.ds(pl.multiple_of((z * xs + column) * 256, 256), 256)
    both = jnp.concatenate([own_ref[:, at], other_ref[:, at]], axis=0)
    return jnp.dot(hidden, both, preferred_element_type=f32).astype(bf16)


def turn_kernel(xs, near_ref, lo_ref, hi_ref, *refs):
    weights, total_ref = refs[:4], refs[4]
    own_ref, other_ref, hidden_ref, out_lo, out_hi = refs[5:]
    half = lo_ref.shape[0]
    far = [lo_ref[z] for z in range(half)] + [hi_ref[z] for z in range(half)]
    total = products([far], [near_ref[xs - 1]], weights, total_ref[...])
    units = total.shape[1] // 2
    gate, up = total[:, :units], total[:, units:]
    hidden = (jax.nn.silu(gate) * up).astype(bf16)
    hidden_ref[...] = hidden
    for z in range(2 * half):
        value = down(hidden, own_ref, other_ref, near_ref[xs - 1], z, xs)
        if z < half:
            out_lo[z] = value
        else:
            out_hi[z - half] = value


def down_kernel(xs, near_ref, hidden_ref, own_ref, other_ref, *outs):
    hidden = hidden_ref[...]
    for out, place in zip(outs, (1, 2, 0)):
        for z in range(out.shape[0]):
            out[z] = down(hidden, own_ref, other_ref, near_ref[place], z, xs)


def merge_kernel(ids_ref, logits_ref, in_ref, out_ref):
    experts, copies = in_ref.shape[0], in_ref.shape[1]
    tok = ids_ref.shape[1]
    chosen, (first, second), low = slot_matrices(ids_ref[...], experts)
    logits = logits_ref[0]
    for n in range(1, logits_ref.shape[0]):
        logits = logits + logits_ref[n]
    logits = jnp.concatenate(
        [logits[i : i + 1, k : k + tok] for i in range(logits.shape[0]) for k in range(0, LANES, tok)], axis=0
    )
    a = jnp.sum(chosen[0] * logits, axis=0, keepdims=True)
    b = jnp.sum(chosen[1] * logits, axis=0, keepdims=True)
    gate = jax.nn.sigmoid(a - b)
    weights = first * gate + second * (1.0 - gate)
    merged = in_ref[:, 0].astype(f32)
    for n in range(1, copies):
        merged = merged + in_ref[:, n].astype(f32)
    merged = merged.reshape(experts * CHUNK, LANES)
    zero = jnp.zeros_like(weights)
    for h in range(2):
        part = jnp.where(low, weights, zero) if h == 0 else jnp.where(low, zero, weights)
        value = lax.dot_general(
            part, merged, (((0,), (0,)), ((), ())), precision=lax.Precision.HIGHEST, preferred_element_type=f32
        )
        out_ref[:, h * LANES : (h + 1) * LANES] = value.astype(bf16)


def block(tokens, router_weight, expert_ids, w_gate, w_up, w_down):
    tok, share = tokens.shape
    xs, zs = lax.axis_size("x"), lax.axis_size("z")
    experts = lax.axis_size(("zh", "yq"))
    sources = experts * 2
    far = sources * zs
    rows = sources * CAP
    half = zs // 2
    assert xs == 4 and share == 256 and zs % 2 == 0
    units = w_gate.shape[2]
    ids = expert_ids.T
    me = lax.axis_index("x")
    near = ((me + jnp.array([0, 1, 3, 2], jnp.int32)) & (xs - 1)).astype(jnp.int32)
    forward = [(i, (i + 1) % xs) for i in range(xs)]
    backward = [(i, (i - 1) % xs) for i in range(xs)]

    def ahead(v):
        return lax.ppermute(v, "x", forward)

    def behind(v):
        return lax.ppermute(v, "x", backward)

    messages, logits = call(
        pack_kernel,
        (
            jax.ShapeDtypeStruct((experts, 2 * zs, CHUNK, LANES), bf16),
            jax.ShapeDtypeStruct((zs * xs, experts * tok // LANES, LANES), f32),
        ),
        10**7,
        10**6,
        mib=60,
        name="pack",
    )(ids, tokens, router_weight.T)
    partial_logits = lax.all_to_all(logits, ("z", "x"), 0, 0, tiled=True)
    arrived = lax.all_to_all(messages.reshape(far, CHUNK, LANES), FAR, 0, 0, tiled=True)

    part = jax.ShapeDtypeStruct((half, rows, share), bf16)
    full = jax.ShapeDtypeStruct((zs, rows, share), bf16)
    own = call(spread_kernel, full, 10**6, 2 * far * CHUNK * LANES * 2, name="spread")(
        arrived.reshape(sources, zs, CHUNK, LANES)
    )

    left = ahead(own)
    right = behind(own)
    swap = [(0, 1), (1, 0)]
    gate_w, up_w, down_w, _ = lax.optimization_barrier((w_gate[0], w_up[0], w_down[0], own))
    gate_o = lax.ppermute(gate_w, "c", swap)
    up_o = lax.ppermute(up_w, "c", swap)
    down_o = lax.ppermute(down_w, "c", swap)
    far_hi = ahead(left[half:])
    far_lo = behind(right[:half])

    smem = pl.BlockSpec(memory_space=pltpu.SMEM)
    vmem = pl.BlockSpec(memory_space=pltpu.VMEM)
    weights = (gate_w, gate_o, up_w, up_o)
    sums = jax.ShapeDtypeStruct((rows, 4 * units), f32)
    flops = 2 * rows * zs * share * 4 * units
    nbytes = zs * share * units * 8 + 2 * half * rows * share * 2

    def gate_up(places, blocks, total):
        more = () if total is None else (total,)
        return call(
            lambda *refs: gate_up_kernel(places, *refs),
            sums,
            flops * len(places),
            nbytes * len(places),
            mib=16,
            in_specs=[smem] + [vmem] * (len(places) + 4 + len(more)),
            name="gate_up",
        )(near, *blocks, *weights, *more)

    total = gate_up((0,), (own,), None)
    total = gate_up((1, 2), (right, left), total)
    hidden, opp_lo, opp_hi = call(
        lambda *refs: turn_kernel(xs, *refs),
        (jax.ShapeDtypeStruct((rows, 2 * units), bf16), part, part),
        2 * flops,
        2 * nbytes,
        mib=20,
        in_specs=[smem] + [vmem] * 9,
        name="turn",
    )(near, far_lo, far_hi, *weights, total, down_w, down_o)

    from_left = ahead(opp_lo)
    from_right = behind(opp_hi)
    to_next, to_prev, mine = call(
        lambda *refs: down_kernel(xs, *refs),
        (full,) * 3,
        2 * flops,
        2 * nbytes,
        mib=12,
        in_specs=[smem] + [vmem] * 3,
        name="down",
    )(near, hidden, down_w, down_o)

    def add(whole, at, term):
        value = (whole[at].astype(f32) + term.astype(f32)).astype(bf16)
        return whole.at[at].set(value)

    from_prev = ahead(add(to_next, slice(0, half), from_left))
    from_next = behind(add(to_prev, slice(half, zs), from_right))

    leaving = call(
        unspread_kernel,
        jax.ShapeDtypeStruct((sources, zs, CHUNK, LANES), bf16),
        10**7,
        4 * far * CHUNK * LANES * 2,
        name="unspread",
    )(mine, from_prev, from_next)
    back = lax.all_to_all(leaving.reshape(far, CHUNK, LANES), FAR, 0, 0, tiled=True)
    return call(
        merge_kernel,
        jax.ShapeDtypeStruct((tok, share), bf16),
        10**7,
        10**6,
        name="merge",
    )(ids, partial_logits, back.reshape(experts, 2 * zs, CHUNK, LANES))


def solution(mesh):
    finer = Mesh(mesh.devices.reshape(2, 4, 2, 2, 6, 4), ("zh", "yq", "yp", "c", "z", "x"))
    dp, tensor = ("zh", "yq", "yp", "c"), ("z", "x")
    return jax.shard_map(
        block,
        mesh=finer,
        in_specs=(
            P(dp, tensor),
            P(tensor, None),
            P(dp, None),
            P(dp, None, tensor),
            P(dp, None, tensor),
            P(dp, tensor, None),
        ),
        out_specs=P(dp, tensor),
        check_vma=False,
    )
```

```python
import jax
import jax.numpy as jnp
from jax import lax
from jax.experimental import pallas as pl
from jax.experimental.pallas import tpu as pltpu
from jax.sharding import Mesh
from jax.sharding import PartitionSpec as P


CAP = 12
LANES = 128
CHUNK = 2 * CAP
FAR = ("zh", "yq", "yp", "z")
f32, bf16 = jnp.float32, jnp.bfloat16


def call(body, out_shape, flops, nbytes, mib=8, **kw):
    return pl.pallas_call(
        body,
        compiler_params=pltpu.CompilerParams(vmem_limit_bytes=mib * 2**20),
        out_shape=out_shape,
        cost_estimate=pl.CostEstimate(flops=flops, bytes_accessed=nbytes, transcendentals=0),
        **kw,
    )


def slot_matrices(ids, experts):
    tok = ids.shape[1]
    which = lax.broadcasted_iota(jnp.int32, (experts, tok), 0)
    chosen = [(which == ids[k : k + 1, :]).astype(f32) for k in range(2)]
    earlier = (
        lax.broadcasted_iota(jnp.int32, (tok, tok), 0) < lax.broadcasted_iota(jnp.int32, (tok, tok), 1)
    ).astype(f32)
    counts = jnp.dot(chosen[0] + chosen[1], earlier, preferred_element_type=f32)
    rows = experts * CHUNK
    flat = lax.broadcasted_iota(jnp.int32, (rows, tok), 0)
    expert = jnp.zeros((rows, tok), jnp.int32)
    for e in range(1, experts):
        expert = expert + (flat >= e * CHUNK).astype(jnp.int32)
    row = flat - expert * CHUNK
    slot = jnp.where(row < 12, row, jnp.where(row < 16, row - 4, row - 16))
    place = expert * CAP + slot
    matrices = []
    for k in range(2):
        rank = jnp.sum(chosen[k] * counts, axis=0, keepdims=True)
        position = ids[k : k + 1, :] * CAP + (rank + 0.5).astype(jnp.int32)
        matrices.append((place == position).astype(f32))
    return chosen, matrices, row < 12


def pack_kernel(ids_ref, tokens_ref, router_ref, out_ref, logits_ref):
    experts, copies = out_ref.shape[0], out_ref.shape[1]
    tok = tokens_ref.shape[0]
    _, (first, second), low = slot_matrices(ids_ref[...], experts)
    placing = first + second
    zero = jnp.zeros_like(placing)
    tokens = tokens_ref[...]
    packed = jnp.dot(
        jnp.where(low, placing, zero).astype(bf16), tokens[:, :LANES], preferred_element_type=f32
    ) + jnp.dot(jnp.where(low, zero, placing).astype(bf16), tokens[:, LANES:], preferred_element_type=f32)
    packed = packed.reshape(experts, CHUNK, LANES).astype(bf16)
    for n in range(copies):
        out_ref[:, n] = packed
    logits = lax.dot_general(router_ref[...], tokens, (((1,), (1,)), ((), ())), preferred_element_type=f32)
    each = LANES // tok
    lines = [jnp.concatenate([logits[i + k : i + k + 1] for k in range(each)], axis=1) for i in range(0, experts, each)]
    lines = jnp.concatenate(lines, axis=0)
    for n in range(logits_ref.shape[0]):
        logits_ref[n] = lines


def spread_kernel(in_ref, out_ref):
    sources, zs = in_ref.shape[0], in_ref.shape[1]
    top = lax.broadcasted_iota(jnp.int32, (8, LANES), 0) < 4
    for z in range(zs):
        for p in range(sources // 2):
            a = in_ref[2 * p, z].astype(f32)
            b = in_ref[2 * p + 1, z].astype(f32)
            ac, bc = a[8:16], b[8:16]
            left = jnp.concatenate([a[0:8], jnp.where(top, ac, pltpu.roll(bc, 4, 0)), b[0:8]], axis=0)
            right = jnp.concatenate([a[16:24], jnp.where(top, pltpu.roll(ac, 4, 0), bc), b[16:24]], axis=0)
            out_ref[z, CHUNK * p : CHUNK * (p + 1), :LANES] = left.astype(bf16)
            out_ref[z, CHUNK * p : CHUNK * (p + 1), LANES:] = right.astype(bf16)


def unspread_kernel(*refs):
    ins, out_ref = refs[:-1], refs[-1]
    sources, zs = out_ref.shape[0], out_ref.shape[1]
    top = lax.broadcasted_iota(jnp.int32, (8, LANES), 0) < 4
    for z in range(zs):
        for p in range(sources // 2):
            total = None
            for ref in ins:
                term = ref[z, CHUNK * p : CHUNK * (p + 1), :].astype(f32)
                total = term if total is None else total + term
            y, w = total[:, :LANES], total[:, LANES:]
            yc, wc = y[8:16], w[8:16]
            a = jnp.concatenate([y[0:8], jnp.where(top, yc, pltpu.roll(wc, 4, 0)), w[0:8]], axis=0)
            b = jnp.concatenate([y[16:24], jnp.where(top, pltpu.roll(yc, 4, 0), wc), w[16:24]], axis=0)
            out_ref[2 * p, z] = a.astype(bf16)
            out_ref[2 * p + 1, z] = b.astype(bf16)


def products(blocks, columns, weights, total):
    xs = 4
    for block, column in zip(blocks, columns):
        for z, rows in enumerate(block):
            share = rows.shape[1]
            at = pl.ds(pl.multiple_of((z * xs + column) * share, share), share)
            both = jnp.concatenate([w[at, :] for w in weights], axis=1)
            term = jnp.dot(rows, both, preferred_element_type=f32)
            total = term if total is None else total + term
    return total


def gate_up_kernel(places, near_ref, *refs):
    parts, weights, more = refs[: len(places)], refs[len(places) : len(places) + 4], refs[len(places) + 4 : -1]
    blocks = [[p[z] for z in range(p.shape[0])] for p in parts]
    refs[-1][...] = products(blocks, [near_ref[n] for n in places], weights, more[0][...] if more else None)


def down(hidden, own_ref, other_ref, column, z, xs):
    at = pl.ds(pl.multiple_of((z * xs + column) * 256, 256), 256)
    both = jnp.concatenate([own_ref[:, at], other_ref[:, at]], axis=0)
    return jnp.dot(hidden, both, preferred_element_type=f32).astype(bf16)


def turn_kernel(xs, near_ref, far_ref, *refs):
    weights, total_ref = refs[:4], refs[4]
    own_ref, other_ref, *outs = refs[5:]
    far = [far_ref[z] for z in range(far_ref.shape[0])]
    total = products([far], [near_ref[xs - 1]], weights, total_ref[...])
    units = total.shape[1] // 2
    gate, up = total[:, :units], total[:, units:]
    hidden = (jax.nn.silu(gate) * up).astype(bf16)
    for n, out in enumerate(outs):
        for z in range(out.shape[0]):
            out[z] = down(hidden, own_ref, other_ref, near_ref[n], z, xs)


def merge_kernel(ids_ref, logits_ref, in_ref, out_ref):
    experts, copies = in_ref.shape[0], in_ref.shape[1]
    tok = ids_ref.shape[1]
    chosen, (first, second), low = slot_matrices(ids_ref[...], experts)
    logits = logits_ref[0]
    for n in range(1, logits_ref.shape[0]):
        logits = logits + logits_ref[n]
    logits = jnp.concatenate(
        [logits[i : i + 1, k : k + tok] for i in range(logits.shape[0]) for k in range(0, LANES, tok)], axis=0
    )
    a = jnp.sum(chosen[0] * logits, axis=0, keepdims=True)
    b = jnp.sum(chosen[1] * logits, axis=0, keepdims=True)
    gate = jax.nn.sigmoid(a - b)
    weights = first * gate + second * (1.0 - gate)
    merged = in_ref[:, 0].astype(f32)
    for n in range(1, copies):
        merged = merged + in_ref[:, n].astype(f32)
    merged = merged.reshape(experts * CHUNK, LANES)
    zero = jnp.zeros_like(weights)
    for h in range(2):
        part = jnp.where(low, weights, zero) if h == 0 else jnp.where(low, zero, weights)
        value = lax.dot_general(
            part, merged, (((0,), (0,)), ((), ())), precision=lax.Precision.HIGHEST, preferred_element_type=f32
        )
        out_ref[:, h * LANES : (h + 1) * LANES] = value.astype(bf16)


def block(tokens, router_weight, expert_ids, w_gate, w_up, w_down):
    tok, share = tokens.shape
    xs, zs = lax.axis_size("x"), lax.axis_size("z")
    experts = lax.axis_size(("zh", "yq"))
    sources = experts * 2
    far = sources * zs
    rows = sources * CAP
    assert xs == 4 and share == 256
    units = w_gate.shape[2]
    ids = expert_ids.T
    me = lax.axis_index("x")
    near = ((me + jnp.array([0, 1, 3, 2], jnp.int32)) & (xs - 1)).astype(jnp.int32)
    forward = [(i, (i + 1) % xs) for i in range(xs)]
    backward = [(i, (i - 1) % xs) for i in range(xs)]

    def ahead(v):
        return lax.ppermute(v, "x", forward)

    def across(v):
        return lax.ppermute(v, "x", [(i, (i + 2) % xs) for i in range(xs)])

    def behind(v):
        return lax.ppermute(v, "x", backward)

    messages, logits = call(
        pack_kernel,
        (
            jax.ShapeDtypeStruct((experts, 2 * zs, CHUNK, LANES), bf16),
            jax.ShapeDtypeStruct((zs * xs, experts * tok // LANES, LANES), f32),
        ),
        10**7,
        10**6,
        mib=60,
        name="pack",
    )(ids, tokens, router_weight.T)
    partial_logits = lax.all_to_all(logits, ("z", "x"), 0, 0, tiled=True)
    arrived = lax.all_to_all(messages.reshape(far, CHUNK, LANES), FAR, 0, 0, tiled=True)

    full = jax.ShapeDtypeStruct((zs, rows, share), bf16)
    own = call(spread_kernel, full, 10**6, 2 * far * CHUNK * LANES * 2, name="spread")(
        arrived.reshape(sources, zs, CHUNK, LANES)
    )

    left = ahead(own)
    right = behind(own)
    opposite = across(own)
    swap = [(0, 1), (1, 0)]
    gate_w, up_w, down_w, _ = lax.optimization_barrier((w_gate[0], w_up[0], w_down[0], own))
    gate_o = lax.ppermute(gate_w, "c", swap)
    up_o = lax.ppermute(up_w, "c", swap)
    down_o = lax.ppermute(down_w, "c", swap)

    smem = pl.BlockSpec(memory_space=pltpu.SMEM)
    vmem = pl.BlockSpec(memory_space=pltpu.VMEM)
    weights = (gate_w, gate_o, up_w, up_o)
    sums = jax.ShapeDtypeStruct((rows, 4 * units), f32)
    flops = 2 * rows * zs * share * 4 * units
    nbytes = zs * share * units * 8 + zs * rows * share * 2

    def gate_up(places, blocks, total):
        more = () if total is None else (total,)
        return call(
            lambda *refs: gate_up_kernel(places, *refs),
            sums,
            flops * len(places),
            nbytes * len(places),
            mib=16,
            in_specs=[smem] + [vmem] * (len(places) + 4 + len(more)),
            name="gate_up",
        )(near, *blocks, *weights, *more)

    total = gate_up((0,), (own,), None)
    total = gate_up((1, 2), (right, left), total)
    mine, to_next, to_prev, to_far = call(
        lambda *refs: turn_kernel(xs, *refs),
        (full,) * xs,
        3 * flops,
        3 * nbytes,
        mib=24,
        in_specs=[smem] + [vmem] * 8,
        name="turn",
    )(near, opposite, *weights, total, down_w, down_o)

    from_far = across(to_far)
    from_prev = ahead(to_next)
    from_next = behind(to_prev)

    leaving = call(
        unspread_kernel,
        jax.ShapeDtypeStruct((sources, zs, CHUNK, LANES), bf16),
        10**7,
        4 * far * CHUNK * LANES * 2,
        name="unspread",
    )(mine, from_prev, from_next, from_far)
    back = lax.all_to_all(leaving.reshape(far, CHUNK, LANES), FAR, 0, 0, tiled=True)
    return call(
        merge_kernel,
        jax.ShapeDtypeStruct((tok, share), bf16),
        10**7,
        10**6,
        name="merge",
    )(ids, partial_logits, back.reshape(experts, 2 * zs, CHUNK, LANES))


def solution(mesh):
    finer = Mesh(mesh.devices.reshape(2, 4, 2, 2, 6, 4), ("zh", "yq", "yp", "c", "z", "x"))
    dp, tensor = ("zh", "yq", "yp", "c"), ("z", "x")
    return jax.shard_map(
        block,
        mesh=finer,
        in_specs=(
            P(dp, tensor),
            P(tensor, None),
            P(dp, None),
            P(dp, None, tensor),
            P(dp, None, tensor),
            P(dp, tensor, None),
        ),
        out_specs=P(dp, tensor),
        check_vma=False,
    )
```

```python
import jax
import jax.numpy as jnp
from jax import lax
from jax.experimental import pallas as pl
from jax.experimental.pallas import tpu as pltpu
from jax.sharding import Mesh
from jax.sharding import PartitionSpec as P


CAP = 12
MIB_GATE, MIB_TURN, MIB_DOWN = 16, 24, 8
LANES = 128
CHUNK = 2 * CAP
FAR = ("zh", "yq", "yp", "z")
f32, bf16 = jnp.float32, jnp.bfloat16


def call(body, out_shape, flops, nbytes, mib=8, **kw):
    return pl.pallas_call(
        body,
        compiler_params=pltpu.CompilerParams(vmem_limit_bytes=mib * 2**20),
        out_shape=out_shape,
        cost_estimate=pl.CostEstimate(flops=flops, bytes_accessed=nbytes, transcendentals=0),
        **kw,
    )


def slot_matrices(ids, experts):
    tok = ids.shape[1]
    which = lax.broadcasted_iota(jnp.int32, (experts, tok), 0)
    chosen = [(which == ids[k : k + 1, :]).astype(f32) for k in range(2)]
    earlier = (
        lax.broadcasted_iota(jnp.int32, (tok, tok), 0) < lax.broadcasted_iota(jnp.int32, (tok, tok), 1)
    ).astype(f32)
    counts = jnp.dot(chosen[0] + chosen[1], earlier, preferred_element_type=f32)
    rows = experts * CHUNK
    flat = lax.broadcasted_iota(jnp.int32, (rows, tok), 0)
    expert = jnp.zeros((rows, tok), jnp.int32)
    for e in range(1, experts):
        expert = expert + (flat >= e * CHUNK).astype(jnp.int32)
    row = flat - expert * CHUNK
    slot = jnp.where(row < 12, row, jnp.where(row < 16, row - 4, row - 16))
    place = expert * CAP + slot
    matrices = []
    for k in range(2):
        rank = jnp.sum(chosen[k] * counts, axis=0, keepdims=True)
        position = ids[k : k + 1, :] * CAP + (rank + 0.5).astype(jnp.int32)
        matrices.append((place == position).astype(f32))
    return chosen, matrices, row < 12


def pack_kernel(ids_ref, tokens_ref, router_ref, out_ref, logits_ref):
    experts, copies = out_ref.shape[0], out_ref.shape[1]
    tok = tokens_ref.shape[0]
    _, (first, second), low = slot_matrices(ids_ref[...], experts)
    placing = first + second
    zero = jnp.zeros_like(placing)
    tokens = tokens_ref[...]
    packed = jnp.dot(
        jnp.where(low, placing, zero).astype(bf16), tokens[:, :LANES], preferred_element_type=f32
    ) + jnp.dot(jnp.where(low, zero, placing).astype(bf16), tokens[:, LANES:], preferred_element_type=f32)
    packed = packed.reshape(experts, CHUNK, LANES).astype(bf16)
    for n in range(copies):
        out_ref[:, n] = packed
    logits = lax.dot_general(router_ref[...], tokens, (((1,), (1,)), ((), ())), preferred_element_type=f32)
    each = LANES // tok
    lines = [jnp.concatenate([logits[i + k : i + k + 1] for k in range(each)], axis=1) for i in range(0, experts, each)]
    lines = jnp.concatenate(lines, axis=0)
    for n in range(logits_ref.shape[0]):
        logits_ref[n] = lines


def spread_kernel(in_ref, out_ref):
    sources, zs = in_ref.shape[0], in_ref.shape[1]
    top = lax.broadcasted_iota(jnp.int32, (8, LANES), 0) < 4
    for z in range(zs):
        for p in range(sources // 2):
            a = in_ref[2 * p, z].astype(f32)
            b = in_ref[2 * p + 1, z].astype(f32)
            ac, bc = a[8:16], b[8:16]
            left = jnp.concatenate([a[0:8], jnp.where(top, ac, pltpu.roll(bc, 4, 0)), b[0:8]], axis=0)
            right = jnp.concatenate([a[16:24], jnp.where(top, pltpu.roll(ac, 4, 0), bc), b[16:24]], axis=0)
            out_ref[z, CHUNK * p : CHUNK * (p + 1), :LANES] = left.astype(bf16)
            out_ref[z, CHUNK * p : CHUNK * (p + 1), LANES:] = right.astype(bf16)


def unspread_kernel(*refs):
    ins, out_ref = refs[:-1], refs[-1]
    sources, zs = out_ref.shape[0], out_ref.shape[1]
    top = lax.broadcasted_iota(jnp.int32, (8, LANES), 0) < 4
    for z in range(zs):
        for p in range(sources // 2):
            total = None
            for ref in ins:
                term = ref[z, CHUNK * p : CHUNK * (p + 1), :].astype(f32)
                total = term if total is None else total + term
            y, w = total[:, :LANES], total[:, LANES:]
            yc, wc = y[8:16], w[8:16]
            a = jnp.concatenate([y[0:8], jnp.where(top, yc, pltpu.roll(wc, 4, 0)), w[0:8]], axis=0)
            b = jnp.concatenate([y[16:24], jnp.where(top, pltpu.roll(yc, 4, 0), wc), w[16:24]], axis=0)
            out_ref[2 * p, z] = a.astype(bf16)
            out_ref[2 * p + 1, z] = b.astype(bf16)


def products(blocks, columns, weights, total):
    xs = 4
    for block, column in zip(blocks, columns):
        for z, rows in enumerate(block):
            share = rows.shape[1]
            at = pl.ds(pl.multiple_of((z * xs + column) * share, share), share)
            both = jnp.concatenate([w[at, :] for w in weights], axis=1)
            term = jnp.dot(rows, both, preferred_element_type=f32)
            total = term if total is None else total + term
    return total


def gate_up_kernel(places, near_ref, *refs):
    parts, weights, more = refs[: len(places)], refs[len(places) : len(places) + 4], refs[len(places) + 4 : -1]
    blocks = [[p[z] for z in range(p.shape[0])] for p in parts]
    refs[-1][...] = products(blocks, [near_ref[n] for n in places], weights, more[0][...] if more else None)


def down(hidden, own_ref, other_ref, column, z, xs):
    at = pl.ds(pl.multiple_of((z * xs + column) * 256, 256), 256)
    both = jnp.concatenate([own_ref[:, at], other_ref[:, at]], axis=0)
    return jnp.dot(hidden, both, preferred_element_type=f32).astype(bf16)


def turn_kernel(xs, near_ref, far_ref, *refs):
    weights, total_ref = refs[:4], refs[4]
    own_ref, other_ref, hidden_ref, *outs = refs[5:]
    far = [far_ref[z] for z in range(far_ref.shape[0])]
    total = products([far], [near_ref[xs - 1]], weights, total_ref[...])
    units = total.shape[1] // 2
    gate, up = total[:, :units], total[:, units:]
    hidden = (jax.nn.silu(gate) * up).astype(bf16)
    hidden_ref[...] = hidden
    for n, out in enumerate(outs):
        for z in range(out.shape[0]):
            out[z] = down(hidden, own_ref, other_ref, near_ref[n + 1], z, xs)


def down_kernel(xs, near_ref, hidden_ref, own_ref, other_ref, out_ref):
    hidden = hidden_ref[...]
    for z in range(out_ref.shape[0]):
        out_ref[z] = down(hidden, own_ref, other_ref, near_ref[0], z, xs)


def merge_kernel(ids_ref, logits_ref, in_ref, out_ref):
    experts, copies = in_ref.shape[0], in_ref.shape[1]
    tok = ids_ref.shape[1]
    chosen, (first, second), low = slot_matrices(ids_ref[...], experts)
    logits = logits_ref[0]
    for n in range(1, logits_ref.shape[0]):
        logits = logits + logits_ref[n]
    logits = jnp.concatenate(
        [logits[i : i + 1, k : k + tok] for i in range(logits.shape[0]) for k in range(0, LANES, tok)], axis=0
    )
    a = jnp.sum(chosen[0] * logits, axis=0, keepdims=True)
    b = jnp.sum(chosen[1] * logits, axis=0, keepdims=True)
    gate = jax.nn.sigmoid(a - b)
    weights = first * gate + second * (1.0 - gate)
    merged = in_ref[:, 0].astype(f32)
    for n in range(1, copies):
        merged = merged + in_ref[:, n].astype(f32)
    merged = merged.reshape(experts * CHUNK, LANES)
    zero = jnp.zeros_like(weights)
    for h in range(2):
        part = jnp.where(low, weights, zero) if h == 0 else jnp.where(low, zero, weights)
        value = lax.dot_general(
            part, merged, (((0,), (0,)), ((), ())), precision=lax.Precision.HIGHEST, preferred_element_type=f32
        )
        out_ref[:, h * LANES : (h + 1) * LANES] = value.astype(bf16)


def block(tokens, router_weight, expert_ids, w_gate, w_up, w_down):
    tok, share = tokens.shape
    xs, zs = lax.axis_size("x"), lax.axis_size("z")
    experts = lax.axis_size(("zh", "yq"))
    sources = experts * 2
    far = sources * zs
    rows = sources * CAP
    assert xs == 4 and share == 256
    units = w_gate.shape[2]
    ids = expert_ids.T
    me = lax.axis_index("x")
    near = ((me + jnp.array([0, 1, 3, 2], jnp.int32)) & (xs - 1)).astype(jnp.int32)
    forward = [(i, (i + 1) % xs) for i in range(xs)]
    backward = [(i, (i - 1) % xs) for i in range(xs)]

    def ahead(v):
        return lax.ppermute(v, "x", forward)

    def across(v):
        return lax.ppermute(v, "x", [(i, (i + 2) % xs) for i in range(xs)])

    def behind(v):
        return lax.ppermute(v, "x", backward)

    messages, logits = call(
        pack_kernel,
        (
            jax.ShapeDtypeStruct((experts, 2 * zs, CHUNK, LANES), bf16),
            jax.ShapeDtypeStruct((zs * xs, experts * tok // LANES, LANES), f32),
        ),
        10**7,
        10**6,
        mib=60,
        name="pack",
    )(ids, tokens, router_weight.T)
    partial_logits = lax.all_to_all(logits, ("z", "x"), 0, 0, tiled=True)
    arrived = lax.all_to_all(messages.reshape(far, CHUNK, LANES), FAR, 0, 0, tiled=True)

    full = jax.ShapeDtypeStruct((zs, rows, share), bf16)
    own = call(spread_kernel, full, 10**6, 2 * far * CHUNK * LANES * 2, name="spread")(
        arrived.reshape(sources, zs, CHUNK, LANES)
    )

    left = ahead(own)
    right = behind(own)
    opposite = across(own)
    swap = [(0, 1), (1, 0)]
    gate_w, up_w, down_w, _ = lax.optimization_barrier((w_gate[0], w_up[0], w_down[0], own))
    gate_o = lax.ppermute(gate_w, "c", swap)
    up_o = lax.ppermute(up_w, "c", swap)
    down_o = lax.ppermute(down_w, "c", swap)

    smem = pl.BlockSpec(memory_space=pltpu.SMEM)
    vmem = pl.BlockSpec(memory_space=pltpu.VMEM)
    weights = (gate_w, gate_o, up_w, up_o)
    sums = jax.ShapeDtypeStruct((rows, 4 * units), f32)
    flops = 2 * rows * zs * share * 4 * units
    nbytes = zs * share * units * 8 + zs * rows * share * 2

    def gate_up(places, blocks, total):
        more = () if total is None else (total,)
        return call(
            lambda *refs: gate_up_kernel(places, *refs),
            sums,
            flops * len(places),
            nbytes * len(places),
            mib=MIB_GATE,
            in_specs=[smem] + [vmem] * (len(places) + 4 + len(more)),
            name="gate_up",
        )(near, *blocks, *weights, *more)

    total = gate_up((0,), (own,), None)
    total = gate_up((1, 2), (right, left), total)
    hidden, to_next, to_prev, to_far = call(
        lambda *refs: turn_kernel(xs, *refs),
        (jax.ShapeDtypeStruct((rows, 2 * units), bf16),) + (full,) * (xs - 1),
        3 * flops,
        3 * nbytes,
        mib=MIB_TURN,
        in_specs=[smem] + [vmem] * 8,
        name="turn",
    )(near, opposite, *weights, total, down_w, down_o)

    from_far = across(to_far)
    from_prev = ahead(to_next)
    from_next = behind(to_prev)
    mine = call(
        lambda *refs: down_kernel(xs, *refs),
        full,
        flops // 2,
        nbytes // 2,
        mib=MIB_DOWN,
        in_specs=[smem] + [vmem] * 3,
        name="down",
    )(near, hidden, down_w, down_o)

    leaving = call(
        unspread_kernel,
        jax.ShapeDtypeStruct((sources, zs, CHUNK, LANES), bf16),
        10**7,
        4 * far * CHUNK * LANES * 2,
        name="unspread",
    )(mine, from_prev, from_next, from_far)
    back = lax.all_to_all(leaving.reshape(far, CHUNK, LANES), FAR, 0, 0, tiled=True)
    return call(
        merge_kernel,
        jax.ShapeDtypeStruct((tok, share), bf16),
        10**7,
        10**6,
        name="merge",
    )(ids, partial_logits, back.reshape(experts, 2 * zs, CHUNK, LANES))


def solution(mesh):
    finer = Mesh(mesh.devices.reshape(2, 4, 2, 2, 6, 4), ("zh", "yq", "yp", "c", "z", "x"))
    dp, tensor = ("zh", "yq", "yp", "c"), ("z", "x")
    return jax.shard_map(
        block,
        mesh=finer,
        in_specs=(
            P(dp, tensor),
            P(tensor, None),
            P(dp, None),
            P(dp, None, tensor),
            P(dp, None, tensor),
            P(dp, tensor, None),
        ),
        out_specs=P(dp, tensor),
        check_vma=False,
    )
```

```python
import jax
import jax.numpy as jnp
from jax import lax
from jax.experimental import pallas as pl
from jax.experimental.pallas import tpu as pltpu
from jax.sharding import Mesh
from jax.sharding import PartitionSpec as P


CAP = 12
MIB_GATE, MIB_TURN, MIB_DOWN = 16, 24, 8
LANES = 128
CHUNK = 2 * CAP
FAR = ("zh", "yq", "yp", "z")
f32, bf16 = jnp.float32, jnp.bfloat16


def call(body, out_shape, flops, nbytes, mib=8, **kw):
    return pl.pallas_call(
        body,
        compiler_params=pltpu.CompilerParams(vmem_limit_bytes=mib * 2**20),
        out_shape=out_shape,
        cost_estimate=pl.CostEstimate(flops=flops, bytes_accessed=nbytes, transcendentals=0),
        **kw,
    )


def slot_matrices(ids, experts):
    tok = ids.shape[1]
    which = lax.broadcasted_iota(jnp.int32, (experts, tok), 0)
    chosen = [(which == ids[k : k + 1, :]).astype(f32) for k in range(2)]
    earlier = (
        lax.broadcasted_iota(jnp.int32, (tok, tok), 0) < lax.broadcasted_iota(jnp.int32, (tok, tok), 1)
    ).astype(f32)
    counts = jnp.dot(chosen[0] + chosen[1], earlier, preferred_element_type=f32)
    rows = experts * CHUNK
    flat = lax.broadcasted_iota(jnp.int32, (rows, tok), 0)
    expert = jnp.zeros((rows, tok), jnp.int32)
    for e in range(1, experts):
        expert = expert + (flat >= e * CHUNK).astype(jnp.int32)
    row = flat - expert * CHUNK
    slot = jnp.where(row < 12, row, jnp.where(row < 16, row - 4, row - 16))
    place = expert * CAP + slot
    matrices = []
    for k in range(2):
        rank = jnp.sum(chosen[k] * counts, axis=0, keepdims=True)
        position = ids[k : k + 1, :] * CAP + (rank + 0.5).astype(jnp.int32)
        matrices.append((place == position).astype(f32))
    return chosen, matrices, row < 12


def pack_kernel(ids_ref, tokens_ref, router_ref, out_ref, logits_ref):
    experts, copies = out_ref.shape[0], out_ref.shape[1]
    tok = tokens_ref.shape[0]
    _, (first, second), low = slot_matrices(ids_ref[...], experts)
    placing = first + second
    zero = jnp.zeros_like(placing)
    tokens = tokens_ref[...]
    packed = jnp.dot(
        jnp.where(low, placing, zero).astype(bf16), tokens[:, :LANES], preferred_element_type=f32
    ) + jnp.dot(jnp.where(low, zero, placing).astype(bf16), tokens[:, LANES:], preferred_element_type=f32)
    packed = packed.reshape(experts, CHUNK, LANES).astype(bf16)
    for n in range(copies):
        out_ref[:, n] = packed
    logits = lax.dot_general(router_ref[...], tokens, (((1,), (1,)), ((), ())), preferred_element_type=f32)
    each = LANES // tok
    lines = [jnp.concatenate([logits[i + k : i + k + 1] for k in range(each)], axis=1) for i in range(0, experts, each)]
    lines = jnp.concatenate(lines, axis=0)
    for n in range(logits_ref.shape[0]):
        logits_ref[n] = lines


def spread_kernel(in_ref, out_ref):
    sources, zs = in_ref.shape[0], in_ref.shape[1]
    top = lax.broadcasted_iota(jnp.int32, (8, LANES), 0) < 4
    for z in range(zs):
        for p in range(sources // 2):
            a = in_ref[2 * p, z].astype(f32)
            b = in_ref[2 * p + 1, z].astype(f32)
            ac, bc = a[8:16], b[8:16]
            left = jnp.concatenate([a[0:8], jnp.where(top, ac, pltpu.roll(bc, 4, 0)), b[0:8]], axis=0)
            right = jnp.concatenate([a[16:24], jnp.where(top, pltpu.roll(ac, 4, 0), bc), b[16:24]], axis=0)
            out_ref[z, CHUNK * p : CHUNK * (p + 1), :LANES] = left.astype(bf16)
            out_ref[z, CHUNK * p : CHUNK * (p + 1), LANES:] = right.astype(bf16)


def unspread_kernel(*refs):
    ins, out_ref = refs[:-1], refs[-1]
    sources, zs = out_ref.shape[0], out_ref.shape[1]
    top = lax.broadcasted_iota(jnp.int32, (8, LANES), 0) < 4
    for z in range(zs):
        for p in range(sources // 2):
            total = None
            for ref in ins:
                term = ref[z, CHUNK * p : CHUNK * (p + 1), :].astype(f32)
                total = term if total is None else total + term
            y, w = total[:, :LANES], total[:, LANES:]
            yc, wc = y[8:16], w[8:16]
            a = jnp.concatenate([y[0:8], jnp.where(top, yc, pltpu.roll(wc, 4, 0)), w[0:8]], axis=0)
            b = jnp.concatenate([y[16:24], jnp.where(top, pltpu.roll(yc, 4, 0), wc), w[16:24]], axis=0)
            out_ref[2 * p, z] = a.astype(bf16)
            out_ref[2 * p + 1, z] = b.astype(bf16)


def products(blocks, columns, weights, total):
    xs = 4
    for block, column in zip(blocks, columns):
        for z, rows in enumerate(block):
            share = rows.shape[1]
            at = pl.ds(pl.multiple_of((z * xs + column) * share, share), share)
            both = jnp.concatenate([w[at, :] for w in weights], axis=1)
            term = jnp.dot(rows, both, preferred_element_type=f32)
            total = term if total is None else total + term
    return total


def gate_up_kernel(places, near_ref, *refs):
    parts, weights, more = refs[: len(places)], refs[len(places) : len(places) + 4], refs[len(places) + 4 : -1]
    blocks = [[p[z] for z in range(p.shape[0])] for p in parts]
    refs[-1][...] = products(blocks, [near_ref[n] for n in places], weights, more[0][...] if more else None)


def down(hidden, own_ref, other_ref, column, z, xs):
    at = pl.ds(pl.multiple_of((z * xs + column) * 256, 256), 256)
    both = jnp.concatenate([own_ref[:, at], other_ref[:, at]], axis=0)
    return jnp.dot(hidden, both, preferred_element_type=f32).astype(bf16)


def turn_kernel(xs, near_ref, lo_ref, hi_ref, *refs):
    weights, total_ref = refs[:4], refs[4]
    own_ref, other_ref, hidden_ref, *outs = refs[5:]
    far = [ref[z] for ref in (lo_ref, hi_ref) for z in range(ref.shape[0])]
    total = products([far], [near_ref[xs - 1]], weights, total_ref[...])
    units = total.shape[1] // 2
    gate, up = total[:, :units], total[:, units:]
    hidden = (jax.nn.silu(gate) * up).astype(bf16)
    hidden_ref[...] = hidden
    for n, out in enumerate(outs):
        for z in range(out.shape[0]):
            out[z] = down(hidden, own_ref, other_ref, near_ref[n + 1], z, xs)


def down_kernel(xs, near_ref, hidden_ref, own_ref, other_ref, out_ref):
    hidden = hidden_ref[...]
    for z in range(out_ref.shape[0]):
        out_ref[z] = down(hidden, own_ref, other_ref, near_ref[0], z, xs)


def merge_kernel(ids_ref, logits_ref, in_ref, out_ref):
    experts, copies = in_ref.shape[0], in_ref.shape[1]
    tok = ids_ref.shape[1]
    chosen, (first, second), low = slot_matrices(ids_ref[...], experts)
    logits = logits_ref[0]
    for n in range(1, logits_ref.shape[0]):
        logits = logits + logits_ref[n]
    logits = jnp.concatenate(
        [logits[i : i + 1, k : k + tok] for i in range(logits.shape[0]) for k in range(0, LANES, tok)], axis=0
    )
    a = jnp.sum(chosen[0] * logits, axis=0, keepdims=True)
    b = jnp.sum(chosen[1] * logits, axis=0, keepdims=True)
    gate = jax.nn.sigmoid(a - b)
    weights = first * gate + second * (1.0 - gate)
    merged = in_ref[:, 0].astype(f32)
    for n in range(1, copies):
        merged = merged + in_ref[:, n].astype(f32)
    merged = merged.reshape(experts * CHUNK, LANES)
    zero = jnp.zeros_like(weights)
    for h in range(2):
        part = jnp.where(low, weights, zero) if h == 0 else jnp.where(low, zero, weights)
        value = lax.dot_general(
            part, merged, (((0,), (0,)), ((), ())), precision=lax.Precision.HIGHEST, preferred_element_type=f32
        )
        out_ref[:, h * LANES : (h + 1) * LANES] = value.astype(bf16)


def block(tokens, router_weight, expert_ids, w_gate, w_up, w_down):
    tok, share = tokens.shape
    xs, zs = lax.axis_size("x"), lax.axis_size("z")
    experts = lax.axis_size(("zh", "yq"))
    sources = experts * 2
    far = sources * zs
    rows = sources * CAP
    assert xs == 4 and share == 256
    units = w_gate.shape[2]
    ids = expert_ids.T
    me = lax.axis_index("x")
    near = ((me + jnp.array([0, 1, 3, 2], jnp.int32)) & (xs - 1)).astype(jnp.int32)
    forward = [(i, (i + 1) % xs) for i in range(xs)]
    backward = [(i, (i - 1) % xs) for i in range(xs)]

    def ahead(v):
        return lax.ppermute(v, "x", forward)

    def across(v):
        return lax.ppermute(v, "x", [(i, (i + 2) % xs) for i in range(xs)])

    def behind(v):
        return lax.ppermute(v, "x", backward)

    messages, logits = call(
        pack_kernel,
        (
            jax.ShapeDtypeStruct((experts, 2 * zs, CHUNK, LANES), bf16),
            jax.ShapeDtypeStruct((zs * xs, experts * tok // LANES, LANES), f32),
        ),
        10**7,
        10**6,
        mib=60,
        name="pack",
    )(ids, tokens, router_weight.T)
    partial_logits = lax.all_to_all(logits, ("z", "x"), 0, 0, tiled=True)
    arrived = lax.all_to_all(messages.reshape(far, CHUNK, LANES), FAR, 0, 0, tiled=True)

    full = jax.ShapeDtypeStruct((zs, rows, share), bf16)
    own = call(spread_kernel, full, 10**6, 2 * far * CHUNK * LANES * 2, name="spread")(
        arrived.reshape(sources, zs, CHUNK, LANES)
    )

    left = ahead(own)
    right = behind(own)
    opposite_lo = across(own[: zs // 2])
    swap = [(0, 1), (1, 0)]
    gate_w, up_w, down_w, _ = lax.optimization_barrier((w_gate[0], w_up[0], w_down[0], own))
    gate_o = lax.ppermute(gate_w, "c", swap)
    up_o = lax.ppermute(up_w, "c", swap)
    down_o = lax.ppermute(down_w, "c", swap)
    opposite_hi = ahead(left[zs // 2 :])

    smem = pl.BlockSpec(memory_space=pltpu.SMEM)
    vmem = pl.BlockSpec(memory_space=pltpu.VMEM)
    weights = (gate_w, gate_o, up_w, up_o)
    sums = jax.ShapeDtypeStruct((rows, 4 * units), f32)
    flops = 2 * rows * zs * share * 4 * units
    nbytes = zs * share * units * 8 + zs * rows * share * 2

    def gate_up(places, blocks, total):
        more = () if total is None else (total,)
        return call(
            lambda *refs: gate_up_kernel(places, *refs),
            sums,
            flops * len(places),
            nbytes * len(places),
            mib=MIB_GATE,
            in_specs=[smem] + [vmem] * (len(places) + 4 + len(more)),
            name="gate_up",
        )(near, *blocks, *weights, *more)

    total = gate_up((0,), (own,), None)
    total = gate_up((1, 2), (right, left), total)
    hidden, to_next, to_prev, to_far = call(
        lambda *refs: turn_kernel(xs, *refs),
        (jax.ShapeDtypeStruct((rows, 2 * units), bf16),) + (full,) * (xs - 1),
        3 * flops,
        3 * nbytes,
        mib=MIB_TURN,
        in_specs=[smem] + [vmem] * 9,
        name="turn",
    )(near, opposite_lo, opposite_hi, *weights, total, down_w, down_o)

    from_far = across(to_far)
    from_prev = ahead(to_next)
    from_next = behind(to_prev)
    mine = call(
        lambda *refs: down_kernel(xs, *refs),
        full,
        flops // 2,
        nbytes // 2,
        mib=MIB_DOWN,
        in_specs=[smem] + [vmem] * 3,
        name="down",
    )(near, hidden, down_w, down_o)

    leaving = call(
        unspread_kernel,
        jax.ShapeDtypeStruct((sources, zs, CHUNK, LANES), bf16),
        10**7,
        4 * far * CHUNK * LANES * 2,
        name="unspread",
    )(mine, from_prev, from_next, from_far)
    back = lax.all_to_all(leaving.reshape(far, CHUNK, LANES), FAR, 0, 0, tiled=True)
    return call(
        merge_kernel,
        jax.ShapeDtypeStruct((tok, share), bf16),
        10**7,
        10**6,
        name="merge",
    )(ids, partial_logits, back.reshape(experts, 2 * zs, CHUNK, LANES))


def solution(mesh):
    finer = Mesh(mesh.devices.reshape(2, 4, 2, 2, 6, 4), ("zh", "yq", "yp", "c", "z", "x"))
    dp, tensor = ("zh", "yq", "yp", "c"), ("z", "x")
    return jax.shard_map(
        block,
        mesh=finer,
        in_specs=(
            P(dp, tensor),
            P(tensor, None),
            P(dp, None),
            P(dp, None, tensor),
            P(dp, None, tensor),
            P(dp, tensor, None),
        ),
        out_specs=P(dp, tensor),
        check_vma=False,
    )
```
